32 devices in a mesh: grp: 8 (over z, x), sp: 4 (over y, core).
Axes of the slice: x: 2, y: 2, z: 4, core: 2. Of those that a mesh axis runs over, the one named last changes fastest.
Arguments:
- query_rows: bfloat16 [4096, 4096], P(('grp', 'sp')), parts along dimension 0, may hold values from -250 to 250
- key_rows: bfloat16 [4096, 1024], P(('grp', 'sp')), parts along dimension 0, may hold values from -4 to 4
- value_rows: bfloat16 [4096, 1024], P(('grp', 'sp')), parts along dimension 0, may hold values from -6 to 6
- out_grad: bfloat16 [4096, 4096], P(('grp', 'sp')), parts along dimension 0, may hold values from -6 to 6
- question_lengths: int32 [64], P('grp'), parts along dimension 0, may hold values from 1 to 128, 256 in all
Outputs:
- query_grad: bfloat16 [4096, 4096], P(('grp', 'sp')), parts along dimension 0
- key_grad: bfloat16 [4096, 1024], P(('grp', 'sp')), parts along dimension 0
- value_grad: bfloat16 [4096, 1024], P(('grp', 'sp')), parts along dimension 0
The draws below stay inside these ranges and needn't reach their ends.
There are 8 independent parts, one for each index of `grp`. The reference program is written for one: setup_inputs(seed, part) draws one part's arguments, and reference() takes and returns one part's arrays. A program takes and returns all parts, laid end to end along the dimension named above; each array names one. Nothing has to cross between parts.
All inputs are finite; a program needn't handle non-finite values.
Results may differ from the reference program's by a relative error of at most 0.033.
Values may be sent and summed in bfloat16 or wider, within the bound.
A program may use at most 128 MiB of HBM per device.

```python
import math
import jax
import jax.numpy as jnp
import numpy as np
from jax import lax

HD = 128
QH = 32
KVH = 8
SEQ = 512
DOC = 256
QMAX = 128
NQ = 8
BLK = 512


def joint_rows(key):
    folded = jax.random.fold_in(key, 11)
    query_key, keys_key = jax.random.split(folded, 2)
    queries = jnp.clip(jax.random.normal(query_key, (SEQ, QH * HD), jnp.float32), -4.0, 4.0)
    keyset = jnp.clip(jax.random.normal(keys_key, (SEQ, KVH * HD), jnp.float32), -4.0, 4.0)
    return (queries, keyset)


def draw_query_rows(key, part):
    return joint_rows(key)[0].astype(jnp.bfloat16)


def draw_key_rows(key, part):
    return joint_rows(key)[1].astype(jnp.bfloat16)


def steps_of(stream_key, extent, pieces, least, high):
    loudness, own = 1.0, jax.random.fold_in(stream_key, 6)
    for axis_at, shards_of in pieces:
        steps = jnp.exp(jax.random.uniform(jax.random.fold_in(own, axis_at), (shards_of,), jnp.float32, least / len(pieces), high / len(pieces)))
        loudness = loudness * jnp.repeat(steps, extent[axis_at] // shards_of).reshape([-1 if axis == axis_at else 1 for axis in range(len(extent))])
    return loudness


def length_profile(count, total, most, lean):
    weights = [(1 << 20) // math.isqrt(rank ** lean) + 1 for rank in range(2, count + 1)]
    surplus, counts = total - most - (count - 1), [1] * (count - 1)
    while surplus > 0:
        movable = [i for i in range(count - 1) if counts[i] < most]
        whole, left = sum([weights[i] for i in movable]), surplus
        for i in movable:
            more = min(most - counts[i], max(1, left * weights[i] // whole), surplus)
            counts[i] = counts[i] + more
            surplus = surplus - more
    return np.array([most] + counts)


def uneven(rng, count, total, bound, slope):
    if count == 2:
        one = jax.random.randint(rng, (), max(1, total - bound), min(bound, total - 1) + 1)
        return jnp.stack([one, total - one])
    sizes = jnp.asarray(length_profile(count, total, bound, slope), jnp.int32)
    couples = (count - 1) // 2
    giver, taker = sizes[1:1 + 2 * couples:2], sizes[2:2 + 2 * couples:2]
    slack = jnp.minimum(giver - 1, bound - taker)
    shifted = jax.random.randint(jax.random.fold_in(rng, 1), (couples,), 0, 1 << 20) % (slack + 1)
    sizes = sizes.at[1:1 + 2 * couples:2].set(giver - shifted).at[2:2 + 2 * couples:2].set(taker + shifted)
    return sizes[jax.random.permutation(jax.random.fold_in(rng, 2), count)]


def gaussian(rng, extent, spread, bound, cuts=(), held_as=jnp.bfloat16):
    level = steps_of(rng, extent, cuts, -0.22, 0.18) if cuts else 1.0
    values = jax.random.normal(rng, extent, jnp.float32) * spread * level
    return jnp.minimum(jnp.maximum(values, -bound), bound).astype(held_as)


def setup_inputs(seed: int = 0, part: int = 0) -> dict:
    seeds = jax.random.split(jax.random.key(seed), 6)
    part_splits = jax.random.split(jax.random.fold_in(seeds[5], part), 6)
    query_rows = draw_query_rows(jax.random.fold_in(jax.random.fold_in(seeds[5], part), 71), part)
    key_rows = draw_key_rows(jax.random.fold_in(jax.random.fold_in(seeds[5], part), 71), part)
    value_rows = gaussian(part_splits[2], (SEQ, KVH * HD), 1.0, 6.0, ((0, 4),))
    out_grad = gaussian(part_splits[3], (SEQ, QH * HD), 1.0, 6.0, ((0, 4),))
    question_lengths = uneven(part_splits[4], NQ, SEQ - DOC, QMAX, 2).astype(jnp.int32)
    return dict(query_rows=query_rows, key_rows=key_rows, value_rows=value_rows, out_grad=out_grad, question_lengths=question_lengths)


MASKED = -1e+30

def rounded(values):
    return lax.optimization_barrier(values.astype(jnp.bfloat16)).astype(jnp.float32)

def segment_ids(question_lengths):
    ends = jnp.cumsum(question_lengths).astype(jnp.int32)
    places = jnp.arange(SEQ, dtype=jnp.int32)
    inside = lax.optimization_barrier(jnp.sum((ends[None, :] <= (places - DOC)[:, None]).astype(jnp.int32), axis=1))
    return jnp.where(places < DOC, -1, inside).astype(jnp.int32)

def reference(query_rows, key_rows, value_rows, out_grad, question_lengths):
    segment = segment_ids(question_lengths)
    places = jnp.arange(SEQ, dtype=jnp.int32)
    group = QH // KVH
    scaling = 1.0 / math.sqrt(HD)
    block_count = SEQ // BLK
    queries = query_rows.reshape(SEQ, KVH, group, HD).transpose(1, 0, 2, 3)
    grads = out_grad.reshape(SEQ, KVH, group, HD).transpose(1, 0, 2, 3)
    keys = key_rows.reshape(SEQ, KVH, HD).transpose(1, 0, 2)
    values = value_rows.reshape(SEQ, KVH, HD).transpose(1, 0, 2)

    def one_group(packed):
        query_group, grad_group, key_group, value_group = packed
        key_float = key_group.astype(jnp.float32)
        value_float = value_group.astype(jnp.float32)

        def step(carry, block):
            key_sum, value_sum = carry
            start = (block * BLK).astype(jnp.int32)
            query_block = lax.dynamic_slice_in_dim(query_group, start, BLK, 0).astype(jnp.float32)
            grad_block = lax.dynamic_slice_in_dim(grad_group, start, BLK, 0).astype(jnp.float32)
            row_places = lax.dynamic_slice_in_dim(places, start, BLK, 0)
            row_segment = lax.dynamic_slice_in_dim(segment, start, BLK, 0)
            visible = (places[None, :] <= row_places[:, None]) & ((places[None, :] < DOC) | (segment[None, :] == row_segment[:, None]))
            scores = jnp.einsum('bgd,sd->gbs', query_block, key_float) * scaling
            scores = jnp.where(visible[None], scores, MASKED)
            peak = lax.optimization_barrier(jnp.max(scores, axis=2))
            log_total = peak + jnp.log(lax.optimization_barrier(jnp.sum(jnp.exp(scores - peak[..., None]), axis=2)))
            probs = jnp.exp(scores - log_total[..., None])
            probs_b = rounded(probs)
            output = rounded(jnp.einsum('gbs,sd->bgd', probs_b, value_float))
            delta = lax.optimization_barrier(jnp.sum(grad_block * output, axis=2)).T
            value_sum = value_sum + jnp.einsum('gbs,bgd->sd', probs_b, grad_block)
            prob_grad = jnp.einsum('bgd,sd->gbs', grad_block, value_float)
            score_grad = rounded(probs * (prob_grad - delta[..., None]))
            query_part = (jnp.einsum('gbs,sd->bgd', score_grad, key_float) * scaling).astype(jnp.bfloat16)
            key_sum = key_sum + jnp.einsum('gbs,bgd->sd', score_grad, query_block) * scaling
            return ((key_sum, value_sum), query_part)
        empty = jnp.zeros((SEQ, HD), jnp.float32)
        sums, query_parts = lax.scan(step, (empty, empty), jnp.arange(block_count, dtype=jnp.int32))
        return (query_parts.reshape(SEQ, group, HD), sums[0].astype(jnp.bfloat16), sums[1].astype(jnp.bfloat16))
    query_all, key_all, value_all = lax.map(one_group, (queries, grads, keys, values))
    query_grad = query_all.transpose(1, 0, 2, 3).reshape(SEQ, QH * HD)
    key_grad = key_all.transpose(1, 0, 2).reshape(SEQ, KVH * HD)
    value_grad = value_all.transpose(1, 0, 2).reshape(SEQ, KVH * HD)
    return (query_grad, key_grad, value_grad)
```

```python
from functools import partial
from functools import reduce
import math

import jax
import jax.numpy as jnp
from jax import lax
from jax.experimental import pallas as pl
from jax.experimental.pallas import tpu as pltpu
from jax.sharding import PartitionSpec as P

HD = 128
QH = 32
KVH = 8


MASKED = -1e30


def widen(rows, copies):
    tokens = rows.shape[0]
    shaped = rows.reshape(tokens, KVH, 1, HD)
    return jnp.broadcast_to(shaped, (tokens, KVH, copies, HD)).reshape(tokens, KVH * copies * HD)


def segment_ids(question_lengths, length, doc_len):
    ends = jnp.cumsum(question_lengths)
    places = jnp.arange(length, dtype=jnp.int32)
    inside = jnp.sum((ends[None, :] <= (places - doc_len)[:, None]).astype(jnp.int32), axis=1)
    return jnp.where(places < doc_len, -1, inside)


def make_scores(query_block, key_block, visible, scaling):
    raw = (
        jnp.einsum("bkgd,skd->kgbs", query_block, key_block, preferred_element_type=jnp.float32)
        * scaling
    )
    return jnp.where(visible[None, None], raw, MASKED)


def weighted_values(probs_b, value_block):
    return jnp.einsum("kgbs,skd->bkgd", probs_b, value_block, preferred_element_type=jnp.float32)


def backward_block(probs, probs_b, delta, grad_block, query_block, key_block, value_block, scaling):
    value_part = jnp.einsum(
        "kgbs,bkgd->skd", probs_b, grad_block, preferred_element_type=jnp.float32
    )
    prob_grad = jnp.einsum(
        "bkgd,skd->kgbs", grad_block, value_block, preferred_element_type=jnp.float32
    )
    score_grad = (probs * (prob_grad - delta[..., None])).astype(jnp.bfloat16)
    query_part = jnp.einsum(
        "kgbs,skd->bkgd", score_grad, key_block, preferred_element_type=jnp.float32
    )
    key_part = (
        jnp.einsum("kgbs,bkgd->skd", score_grad, query_block, preferred_element_type=jnp.float32)
        * scaling
    )
    return (query_part, key_part, value_part)


def on_device(query_rows, key_rows, value_rows, out_grad, question_lengths):
    devices = lax.axis_size("sp")
    tokens = query_rows.shape[0]
    length = tokens * devices
    doc_len = length // 2
    block_len = min(512, length)
    block_count = length // block_len
    scaling = 1.0 / math.sqrt(HD)
    copies = max(KVH, devices) // KVH
    keys_local, values_local = (
        lax.all_to_all(widen(key_rows, copies), "sp", split_axis=1, concat_axis=0, tiled=True),
        lax.all_to_all(widen(value_rows, copies), "sp", split_axis=1, concat_axis=0, tiled=True),
    )
    queries_local, grads_local = (
        lax.all_to_all(query_rows, "sp", split_axis=1, concat_axis=0, tiled=True),
        lax.all_to_all(out_grad, "sp", split_axis=1, concat_axis=0, tiled=True),
    )
    key_heads = KVH * copies // devices
    per_group = QH // devices // key_heads
    queries = queries_local.reshape(length, key_heads, per_group, HD)
    grads = grads_local.reshape(length, key_heads, per_group, HD)
    keys = keys_local.reshape(length, key_heads, HD)
    values = values_local.reshape(length, key_heads, HD)
    segment = segment_ids(question_lengths, length, doc_len)
    places = jnp.arange(length, dtype=jnp.int32)
    query_shape = (block_len, key_heads, per_group, HD)
    key_shape = (block_len, key_heads, HD)
    key_sums = [jnp.zeros(key_shape, jnp.float32)] * block_count
    value_sums = [jnp.zeros(key_shape, jnp.float32)] * block_count
    query_parts = []
    for row_block in range(block_count):
        row_start = row_block * block_len
        query_block = queries[row_start : row_start + block_len]
        grad_block = grads[row_start : row_start + block_len]
        row_places = places[row_start : row_start + block_len]
        row_segment = segment[row_start : row_start + block_len]
        needs = []
        scores = []
        for col_block in range(row_block + 1):
            col_start = col_block * block_len
            col_places = places[col_start : col_start + block_len]
            col_segment = segment[col_start : col_start + block_len]
            visible = (col_places[None, :] <= row_places[:, None]) & (
                (col_places[None, :] < doc_len) | (col_segment[None, :] == row_segment[:, None])
            )
            needed = True
            needs.append(needed)
            scores.append(
                make_scores(query_block, keys[col_start : col_start + block_len], visible, scaling)
            )
        peak = reduce(jnp.maximum, [jnp.max(score, axis=3) for score in scores])
        total = reduce(
            jnp.add, [jnp.sum(jnp.exp(score - peak[..., None]), axis=3) for score in scores]
        )
        log_total = peak + jnp.log(total)
        probs = [jnp.exp(score - log_total[..., None]) for score in scores]
        probs_low = [single.astype(jnp.bfloat16) for single in probs]
        output = jnp.zeros(query_shape, jnp.float32)
        for col_block in range(row_block + 1):
            col_start = col_block * block_len
            output = output + weighted_values(
                probs_low[col_block], values[col_start : col_start + block_len]
            )
        output_low = output.astype(jnp.bfloat16)
        delta = jnp.einsum(
            "bkgd,bkgd->kgb", grad_block, output_low, preferred_element_type=jnp.float32
        )
        query_sum = jnp.zeros(query_shape, jnp.float32)
        for col_block in range(row_block + 1):
            col_start = col_block * block_len
            action = partial(
                backward_block,
                probs[col_block],
                probs_low[col_block],
                delta,
                grad_block,
                query_block,
                keys[col_start : col_start + block_len],
                values[col_start : col_start + block_len],
                scaling,
            )
            query_part, key_part, value_part = action()
            query_sum = query_sum + query_part
            key_sums[col_block] = key_sums[col_block] + key_part
            value_sums[col_block] = value_sums[col_block] + value_part
        query_parts.append((query_sum * scaling).astype(jnp.bfloat16))
    query_local = jnp.concatenate(query_parts, axis=0).reshape(length, key_heads * per_group * HD)
    key_local = jnp.concatenate(key_sums, axis=0).reshape(length, key_heads * HD)
    value_local = jnp.concatenate(value_sums, axis=0).reshape(length, key_heads * HD)
    query_grad = lax.all_to_all(query_local, "sp", split_axis=0, concat_axis=1, tiled=True)
    key_back, value_back = (
        lax.all_to_all(key_local, "sp", split_axis=0, concat_axis=1, tiled=True),
        lax.all_to_all(value_local, "sp", split_axis=0, concat_axis=1, tiled=True),
    )
    key_grad = (
        jnp.sum(key_back.reshape(tokens, KVH, copies, HD), axis=2)
        .reshape(tokens, KVH * HD)
        .astype(jnp.bfloat16)
    )
    value_grad = (
        jnp.sum(value_back.reshape(tokens, KVH, copies, HD), axis=2)
        .reshape(tokens, KVH * HD)
        .astype(jnp.bfloat16)
    )
    return (query_grad, key_grad, value_grad)


MESH = pl.DeviceIdType.MESH
CORES = 2


def dot(left, right, left_dim, right_dim):
    return lax.dot_general(
        left, right, (((left_dim,), (right_dim,)), ((), ())), preferred_element_type=jnp.float32
    )


def flip(tile):
    return jnp.transpose(tile.astype(jnp.float32))


def pair_kernel(
    tokens, heads, group, lengths_hbm, q_hbm, g_hbm, k_hbm, v_hbm, dq, dk, dv,
    qx, gx, kx, vx, kd, vd, bias, probs, grads, probs_low, score_low, acc, part, away, back,
    lengths_ref, lengths_sem, kv_sem, own_sem, kv_swap_send, kv_swap_recv, swap_send, swap_recv,
    doc_send, doc_recv, term_send, term_recv, part_send, part_recv, out_send, out_recv,
):
    me = lax.axis_index("sp")
    chip = me // CORES
    core = lax.rem(me, CORES)
    other = 1 - core
    sibling = chip * CORES + other
    rows = tokens * CORES
    wide = group * HD
    pairs = group // 2
    scaling = 1.0 / math.sqrt(HD)

    def cols(half, j, width):
        return pl.ds(pl.multiple_of((half * heads + j) * width, width), width)

    def remote(src, dst, send, recv, device):
        return pltpu.make_async_remote_copy(
            src_ref=src, dst_ref=dst, send_sem=send, recv_sem=recv,
            device_id={"sp": device}, device_id_type=MESH,
        )

    kv_own = [
        pltpu.make_async_copy(src, dst.at[core], kv_sem.at[i])
        for i, (src, dst) in enumerate(((k_hbm, kx), (v_hbm, vx)))
    ]

    def own_copies(j, which):
        half = (core, other)[which]
        return [
            pltpu.make_async_copy(
                src.at[:, cols(half, j, wide)], dst.at[core, :, cols(half, j, wide)],
                own_sem.at[i, which, j],
            )
            for i, (src, dst) in enumerate(((q_hbm, qx), (g_hbm, gx)))
        ]

    kv_half = pl.ds(pl.multiple_of(other * heads * HD, heads * HD), heads * HD)
    kv_swap = [
        remote(
            ref.at[core, :, kv_half], ref.at[core, :, kv_half],
            kv_swap_send.at[i], kv_swap_recv.at[i], sibling,
        )
        for i, ref in enumerate((kx, vx))
    ]

    def swap_copies(j):
        return [
            remote(
                ref.at[core, :, cols(other, j, wide)], ref.at[core, :, cols(other, j, wide)],
                swap_send.at[i, j], swap_recv.at[i, j], sibling,
            )
            for i, ref in enumerate((qx, gx))
        ]

    def doc_copies(j, i, source_core):
        from_rows = pl.ds(pl.multiple_of(source_core * tokens, tokens), tokens)
        src, dst = ((kx, kd), (vx, vd))[i]
        return [
            remote(
                src.at[source_core, :, cols(half, j, HD)], dst.at[j, from_rows],
                doc_send.at[half, i, j], doc_recv.at[source_core, i, j], CORES + half,
            )
            for half in range(CORES)
        ]

    def term_copies(j, i, half):
        return [
            remote(
                away.at[i, j, pl.ds(keeper * tokens, tokens)], back.at[i, half, j],
                term_send.at[i, keeper, j], term_recv.at[i, half, j], keeper,
            )
            for keeper in range(CORES)
        ]

    def part_copy(j, i):
        return remote(
            part.at[i, j], acc.at[i, core, j], part_send.at[i, j], part_recv.at[i, j], sibling
        )

    def out_copy(j, i):
        ref, width = ((dq, wide), (dk, HD), (dv, HD))[i]
        view = ref.at[other, :, cols(core, j, width)]
        return remote(view, view, out_send.at[i, j], out_recv.at[i, j], sibling)

    lengths_copy = pltpu.make_async_copy(lengths_hbm, lengths_ref, lengths_sem)
    for copy in kv_own:
        copy.start()
    lengths_copy.start()
    for j in range(heads):
        for copy in own_copies(j, 1) + own_copies(j, 0):
            copy.start()

    barrier = pltpu.get_barrier_semaphore()
    for step in range(1, 2 * CORES):
        pl.semaphore_signal(
            barrier, inc=1, device_id={"sp": lax.rem(me + step, 2 * CORES)}, device_id_type=MESH
        )
    pl.semaphore_wait(barrier, 2 * CORES - 1)
    for copy in kv_own:
        copy.wait()

    @pl.when(chip == 0)
    def _():
        for j in range(heads):
            for i in range(2):
                for copy in doc_copies(j, i, core):
                    copy.start()

    for copy in kv_swap:
        copy.start()
    for j in range(heads):
        for copy in own_copies(j, 1):
            copy.wait()
        for copy in swap_copies(j):
            copy.start()

    lengths_copy.wait()
    places = chip * rows + lax.broadcasted_iota(jnp.int32, (1, rows), 1)
    doc_len = rows
    asked = places - doc_len
    start = jnp.zeros((1, rows), jnp.int32)
    end = jnp.int32(0)
    for c in range(lengths_ref.shape[0]):
        end = end + lengths_ref[c]
        start = jnp.where(end <= asked, end, start)
    first = jnp.where(asked < 0, 0, start + doc_len)
    key_places = chip * rows + lax.broadcasted_iota(jnp.int32, (rows, rows), 0)
    query_places = chip * rows + lax.broadcasted_iota(jnp.int32, (rows, rows), 1)
    seen = (key_places <= query_places) & (key_places >= first)
    bias[...] = jnp.where(seen, 0.0, MASKED)

    for copy in kv_swap:
        copy.wait()

    tiles = [(a, p) for a in range(CORES) for p in range(pairs)]

    def head_cols(j, h):
        return pl.ds(pl.multiple_of((core * heads + j) * wide + h * HD, HD), HD)

    def block(ref, j, a, p):
        return jnp.concatenate(
            [ref[a, :, head_cols(j, 2 * p)], ref[a, :, head_cols(j, 2 * p + 1)]], axis=0
        )

    def whole(ref, j, first_a):
        return jnp.concatenate(
            [block(ref, j, a, p) for a, p in tiles if a >= first_a], axis=0
        )

    def own(ref, j, a):
        return ref[: a + 1, :, cols(core, j, HD)].reshape((a + 1) * tokens, HD)

    def span(n):
        return slice(n * rows, (n + 1) * rows)

    def arrive(j):
        for copy in own_copies(j, 0) + swap_copies(j):
            copy.wait()

    def own_scores(j, low):
        for n, (a, p) in enumerate(tiles):
            seen_keys = (a + 1) * tokens
            raw = dot(own(kx, j, a), block(qx, j, a, p), 1, 1)
            mask = bias[:seen_keys, a * tokens : (a + 1) * tokens]
            probs[n, low : low + seen_keys] = raw + jnp.concatenate([mask, mask], axis=1)

    def own_grads(j, low):
        for n, (a, p) in enumerate(tiles):
            grads[n, low : low + (a + 1) * tokens] = dot(own(vx, j, a), block(gx, j, a, p), 1, 1)

    def normalize(j, low):
        for n, (a, p) in enumerate(tiles):
            extent = low + (a + 1) * tokens
            raw = probs[n, low:extent]
            if low:
                raw = jnp.concatenate([dot(kd[j], block(qx, j, a, p), 1, 1), raw], axis=0)
            peak = jnp.max(raw, axis=0, keepdims=True)
            weight = jnp.exp2((raw - peak) * (scaling * math.log2(math.e)))
            total = jnp.sum(weight, axis=0, keepdims=True)
            single = weight * (1.0 / total)
            probs[n, :extent] = single
            probs_low[:extent, span(n)] = single.astype(jnp.bfloat16)

    def differentiate(j, low):
        for n, (a, p) in enumerate(tiles):
            extent = low + (a + 1) * tokens
            single = probs[n, :extent]
            grad = grads[n, low:extent]
            if low:
                grad = jnp.concatenate([dot(vd[j], block(gx, j, a, p), 1, 1), grad], axis=0)
            delta = jnp.sum(single * grad, axis=0, keepdims=True)
            score_low[:extent, span(n)] = (single * (grad - delta)).astype(jnp.bfloat16)

    def sum_over(low_ref, ref, j, low):
        everyone = whole(ref, j, 0)
        return [
            dot(
                low_ref[low + b * tokens : low + (b + 1) * tokens, b * pairs * rows :],
                everyone[b * pairs * rows :], 1, 0,
            )
            for b in range(CORES)
        ]

    def query_grads(j, low):
        keys = own(kx, j, CORES - 1)
        if low:
            keys = jnp.concatenate([kd[j], keys], axis=0)
        keys_flat = flip(keys).astype(jnp.bfloat16)
        for n, (a, p) in enumerate(tiles):
            extent = low + (a + 1) * tokens
            flat = dot(keys_flat[:, :extent], score_low[:extent, span(n)], 1, 0) * scaling
            for h in range(2):
                dq[a, :, head_cols(j, 2 * p + h)] = jnp.transpose(
                    flat[:, h * tokens : (h + 1) * tokens]
                ).astype(jnp.bfloat16)

    @pl.when(chip == 0)
    def _():
        def keep(i, j, low, high):
            acc[i, core, j] = jnp.where(core == 0, low, high)
            part[i, j] = jnp.where(core == 0, high, low)
            part_copy(j, i).start()

        def step(j, carry):
            arrive(j)
            own_scores(j, 0)
            own_grads(j, 0)
            normalize(j, 0)
            low, high = sum_over(probs_low, gx, j, 0)
            keep(1, j, low, high)
            differentiate(j, 0)
            low, high = sum_over(score_low, qx, j, 0)
            keep(0, j, low * scaling, high * scaling)
            query_grads(j, 0)
            out_copy(j, 0).start()
            return carry

        lax.fori_loop(0, heads, step, 0)

        def finish(j, carry):
            for i in (1, 0):
                part_copy(j, i).wait()
                for half in range(CORES):
                    term_copies(j, i, half)[0].wait_recv()
                    total = acc[i, half, j] + back[i, half, j].astype(jnp.float32)
                    (dk, dv)[i][core, :, cols(half, j, HD)] = total.astype(jnp.bfloat16)
            return carry

        lax.fori_loop(0, heads, finish, 0)
        for j in range(heads):
            for i in range(2):
                for copy in doc_copies(j, i, core):
                    copy.wait_send()
            out_copy(j, 0).wait()

    @pl.when(chip == 1)
    def _():
        def step(j, carry):
            arrive(j)
            own_scores(j, rows)
            for source_core in range(CORES):
                doc_copies(j, 0, source_core)[0].wait_recv()
            normalize(j, rows)
            away[1, j] = dot(probs_low[:rows], whole(gx, j, 0), 1, 0).astype(jnp.bfloat16)
            for copy in term_copies(j, 1, core):
                copy.start()
            own_grads(j, rows)
            for a, total in enumerate(sum_over(probs_low, gx, j, rows)):
                dv[a, :, cols(core, j, HD)] = total.astype(jnp.bfloat16)
            for source_core in range(CORES):
                doc_copies(j, 1, source_core)[0].wait_recv()
            differentiate(j, rows)
            away[0, j] = (dot(score_low[:rows], whole(qx, j, 0), 1, 0) * scaling).astype(
                jnp.bfloat16
            )
            for copy in term_copies(j, 0, core):
                copy.start()
            for a, total in enumerate(sum_over(score_low, qx, j, rows)):
                dk[a, :, cols(core, j, HD)] = (total * scaling).astype(jnp.bfloat16)
            query_grads(j, rows)
            for i in range(3):
                out_copy(j, i).start()
            return carry

        lax.fori_loop(0, heads, step, 0)
        for j in range(heads):
            for i in range(2):
                for copy in term_copies(j, i, core):
                    copy.wait_send()
            for i in range(3):
                out_copy(j, i).wait()


def publish_kernel(dq_in, dk_in, dv_in, dq_out, dk_out, dv_out, sem):
    core = lax.rem(lax.axis_index("sp"), CORES)
    copies = [
        pltpu.make_async_copy(src.at[core], dst, sem.at[i])
        for i, (src, dst) in enumerate(((dq_in, dq_out), (dk_in, dk_out), (dv_in, dv_out)))
    ]
    for copy in copies:
        copy.start()
    for copy in copies:
        copy.wait()


def on_pairs(query_rows, key_rows, value_rows, out_grad, question_lengths):
    tokens = query_rows.shape[0]
    heads = KVH // CORES
    group = QH // KVH
    rows = tokens * CORES
    low, wide = jnp.bfloat16, jnp.float32
    vmem, sems = pltpu.VMEM, lambda *shape: pltpu.SemaphoreType.DMA(shape)
    anywhere = pl.BlockSpec(memory_space=pl.ANY)
    tiles = group * CORES // 2
    grads = pl.pallas_call(
        partial(pair_kernel, tokens, heads, group),
        out_shape=tuple(
            pltpu.VMEM((CORES,) + array.shape, low) for array in (query_rows, key_rows, value_rows)
        ),
        in_specs=[anywhere] * 5,
        out_specs=(pl.BlockSpec(memory_space=pltpu.VMEM),) * 3,
        scratch_shapes=[
            vmem((CORES,) + query_rows.shape, low),
            vmem((CORES,) + query_rows.shape, low),
            vmem((CORES,) + key_rows.shape, low),
            vmem((CORES,) + key_rows.shape, low),
            vmem((heads, rows, HD), low),
            vmem((heads, rows, HD), low),
            vmem((rows, rows), wide),
            vmem((tiles, 2 * rows, rows), wide),
            vmem((tiles, 2 * rows, rows), wide),
            vmem((2 * rows, tiles * rows), low),
            vmem((2 * rows, tiles * rows), low),
            vmem((2, CORES, heads, tokens, HD), wide),
            vmem((2, heads, tokens, HD), wide),
            vmem((2, heads, rows, HD), low),
            vmem((2, CORES, heads, tokens, HD), low),
            pltpu.SMEM(question_lengths.shape, jnp.int32),
            pltpu.SemaphoreType.DMA,
            sems(2),
            sems(2, CORES, heads),
            sems(2),
            sems(2),
            sems(2, heads),
            sems(2, heads),
            sems(CORES, 2, heads),
            sems(CORES, 2, heads),
            sems(2, CORES, heads),
            sems(2, CORES, heads),
            sems(2, heads),
            sems(2, heads),
            sems(3, heads),
            sems(3, heads),
        ],
        compiler_params=pltpu.CompilerParams(
            collective_id=0, has_side_effects=True,
        ),
    )(question_lengths, query_rows, out_grad, key_rows, value_rows)
    return pl.pallas_call(
        publish_kernel,
        out_shape=tuple(
            jax.ShapeDtypeStruct(array.shape, low) for array in (query_rows, key_rows, value_rows)
        ),
        in_specs=[anywhere] * 3,
        out_specs=(anywhere,) * 3,
        scratch_shapes=[sems(3)],
        compiler_params=pltpu.CompilerParams(has_side_effects=True, vmem_limit_bytes=1024 * 1024),
    )(*grads)


def solution(mesh):
    body = on_pairs if mesh.shape["sp"] == 2 * CORES else on_device
    return jax.shard_map(
        body,
        mesh=mesh,
        in_specs=(
            P(("grp", "sp"), None),
            P(("grp", "sp"), None),
            P(("grp", "sp"), None),
            P(("grp", "sp"), None),
            P("grp"),
        ),
        out_specs=(P(("grp", "sp"), None), P(("grp", "sp"), None), P(("grp", "sp"), None)),
        check_vma=False,
    )
```

```python
from functools import partial
from functools import reduce
import math

import jax
import jax.numpy as jnp
from jax import lax
from jax.experimental import pallas as pl
from jax.experimental.pallas import tpu as pltpu
from jax.sharding import PartitionSpec as P

HD = 128
QH = 32
KVH = 8


MASKED = -1e30


def widen(rows, copies):
    tokens = rows.shape[0]
    shaped = rows.reshape(tokens, KVH, 1, HD)
    return jnp.broadcast_to(shaped, (tokens, KVH, copies, HD)).reshape(tokens, KVH * copies * HD)


def segment_ids(question_lengths, length, doc_len):
    ends = jnp.cumsum(question_lengths)
    places = jnp.arange(length, dtype=jnp.int32)
    inside = jnp.sum((ends[None, :] <= (places - doc_len)[:, None]).astype(jnp.int32), axis=1)
    return jnp.where(places < doc_len, -1, inside)


def make_scores(query_block, key_block, visible, scaling):
    raw = (
        jnp.einsum("bkgd,skd->kgbs", query_block, key_block, preferred_element_type=jnp.float32)
        * scaling
    )
    return jnp.where(visible[None, None], raw, MASKED)


def weighted_values(probs_b, value_block):
    return jnp.einsum("kgbs,skd->bkgd", probs_b, value_block, preferred_element_type=jnp.float32)


def backward_block(probs, probs_b, delta, grad_block, query_block, key_block, value_block, scaling):
    value_part = jnp.einsum(
        "kgbs,bkgd->skd", probs_b, grad_block, preferred_element_type=jnp.float32
    )
    prob_grad = jnp.einsum(
        "bkgd,skd->kgbs", grad_block, value_block, preferred_element_type=jnp.float32
    )
    score_grad = (probs * (prob_grad - delta[..., None])).astype(jnp.bfloat16)
    query_part = jnp.einsum(
        "kgbs,skd->bkgd", score_grad, key_block, preferred_element_type=jnp.float32
    )
    key_part = (
        jnp.einsum("kgbs,bkgd->skd", score_grad, query_block, preferred_element_type=jnp.float32)
        * scaling
    )
    return (query_part, key_part, value_part)


def on_device(query_rows, key_rows, value_rows, out_grad, question_lengths):
    devices = lax.axis_size("sp")
    tokens = query_rows.shape[0]
    length = tokens * devices
    doc_len = length // 2
    block_len = min(512, length)
    block_count = length // block_len
    scaling = 1.0 / math.sqrt(HD)
    copies = max(KVH, devices) // KVH
    keys_local, values_local = (
        lax.all_to_all(widen(key_rows, copies), "sp", split_axis=1, concat_axis=0, tiled=True),
        lax.all_to_all(widen(value_rows, copies), "sp", split_axis=1, concat_axis=0, tiled=True),
    )
    queries_local, grads_local = (
        lax.all_to_all(query_rows, "sp", split_axis=1, concat_axis=0, tiled=True),
        lax.all_to_all(out_grad, "sp", split_axis=1, concat_axis=0, tiled=True),
    )
    key_heads = KVH * copies // devices
    per_group = QH // devices // key_heads
    queries = queries_local.reshape(length, key_heads, per_group, HD)
    grads = grads_local.reshape(length, key_heads, per_group, HD)
    keys = keys_local.reshape(length, key_heads, HD)
    values = values_local.reshape(length, key_heads, HD)
    segment = segment_ids(question_lengths, length, doc_len)
    places = jnp.arange(length, dtype=jnp.int32)
    query_shape = (block_len, key_heads, per_group, HD)
    key_shape = (block_len, key_heads, HD)
    key_sums = [jnp.zeros(key_shape, jnp.float32)] * block_count
    value_sums = [jnp.zeros(key_shape, jnp.float32)] * block_count
    query_parts = []
    for row_block in range(block_count):
        row_start = row_block * block_len
        query_block = queries[row_start : row_start + block_len]
        grad_block = grads[row_start : row_start + block_len]
        row_places = places[row_start : row_start + block_len]
        row_segment = segment[row_start : row_start + block_len]
        needs = []
        scores = []
        for col_block in range(row_block + 1):
            col_start = col_block * block_len
            col_places = places[col_start : col_start + block_len]
            col_segment = segment[col_start : col_start + block_len]
            visible = (col_places[None, :] <= row_places[:, None]) & (
                (col_places[None, :] < doc_len) | (col_segment[None, :] == row_segment[:, None])
            )
            needed = True
            needs.append(needed)
            scores.append(
                make_scores(query_block, keys[col_start : col_start + block_len], visible, scaling)
            )
        peak = reduce(jnp.maximum, [jnp.max(score, axis=3) for score in scores])
        total = reduce(
            jnp.add, [jnp.sum(jnp.exp(score - peak[..., None]), axis=3) for score in scores]
        )
        log_total = peak + jnp.log(total)
        probs = [jnp.exp(score - log_total[..., None]) for score in scores]
        probs_low = [single.astype(jnp.bfloat16) for single in probs]
        output = jnp.zeros(query_shape, jnp.float32)
        for col_block in range(row_block + 1):
            col_start = col_block * block_len
            output = output + weighted_values(
                probs_low[col_block], values[col_start : col_start + block_len]
            )
        output_low = output.astype(jnp.bfloat16)
        delta = jnp.einsum(
            "bkgd,bkgd->kgb", grad_block, output_low, preferred_element_type=jnp.float32
        )
        query_sum = jnp.zeros(query_shape, jnp.float32)
        for col_block in range(row_block + 1):
            col_start = col_block * block_len
            action = partial(
                backward_block,
                probs[col_block],
                probs_low[col_block],
                delta,
                grad_block,
                query_block,
                keys[col_start : col_start + block_len],
                values[col_start : col_start + block_len],
                scaling,
            )
            query_part, key_part, value_part = action()
            query_sum = query_sum + query_part
            key_sums[col_block] = key_sums[col_block] + key_part
            value_sums[col_block] = value_sums[col_block] + value_part
        query_parts.append((query_sum * scaling).astype(jnp.bfloat16))
    query_local = jnp.concatenate(query_parts, axis=0).reshape(length, key_heads * per_group * HD)
    key_local = jnp.concatenate(key_sums, axis=0).reshape(length, key_heads * HD)
    value_local = jnp.concatenate(value_sums, axis=0).reshape(length, key_heads * HD)
    query_grad = lax.all_to_all(query_local, "sp", split_axis=0, concat_axis=1, tiled=True)
    key_back, value_back = (
        lax.all_to_all(key_local, "sp", split_axis=0, concat_axis=1, tiled=True),
        lax.all_to_all(value_local, "sp", split_axis=0, concat_axis=1, tiled=True),
    )
    key_grad = (
        jnp.sum(key_back.reshape(tokens, KVH, copies, HD), axis=2)
        .reshape(tokens, KVH * HD)
        .astype(jnp.bfloat16)
    )
    value_grad = (
        jnp.sum(value_back.reshape(tokens, KVH, copies, HD), axis=2)
        .reshape(tokens, KVH * HD)
        .astype(jnp.bfloat16)
    )
    return (query_grad, key_grad, value_grad)


MESH = pl.DeviceIdType.MESH
CORES = 2


def dot(left, right, left_dim, right_dim):
    return lax.dot_general(
        left, right, (((left_dim,), (right_dim,)), ((), ())), preferred_element_type=jnp.float32
    )


def flip(tile):
    return jnp.transpose(tile.astype(jnp.float32))


def pair_body(
    tokens, heads, group, lengths_hbm, q_hbm, g_hbm, k_hbm, v_hbm, dq, dk, dv,
    qx, gx, kx, vx, kd, vd, bias, probs, grads, probs_low, score_low, acc, part, away, back,
    lengths_ref, lengths_sem, kv_sem, own_sem, kv_swap_send, kv_swap_recv, swap_send, swap_recv,
    doc_send, doc_recv, term_send, term_recv, part_send, part_recv, out_send, out_recv,
):
    me = lax.axis_index("sp")
    chip = me // CORES
    core = lax.rem(me, CORES)
    other = 1 - core
    sibling = chip * CORES + other
    rows = tokens * CORES
    wide = group * HD
    pairs = group // 2
    scaling = 1.0 / math.sqrt(HD)

    def cols(half, j, width):
        return pl.ds(pl.multiple_of((half * heads + j) * width, width), width)

    def remote(src, dst, send, recv, device):
        return pltpu.make_async_remote_copy(
            src_ref=src, dst_ref=dst, send_sem=send, recv_sem=recv,
            device_id={"sp": device}, device_id_type=MESH,
        )

    kv_own = [
        pltpu.make_async_copy(src, dst.at[core], kv_sem.at[i])
        for i, (src, dst) in enumerate(((k_hbm, kx), (v_hbm, vx)))
    ]

    def own_copies(j, which):
        half = (core, other)[which]
        return [
            pltpu.make_async_copy(
                src.at[:, cols(half, j, wide)], dst.at[core, :, cols(half, j, wide)],
                own_sem.at[i, which, j],
            )
            for i, (src, dst) in enumerate(((q_hbm, qx), (g_hbm, gx)))
        ]

    kv_half = pl.ds(pl.multiple_of(other * heads * HD, heads * HD), heads * HD)
    kv_swap = [
        remote(
            ref.at[core, :, kv_half], ref.at[core, :, kv_half],
            kv_swap_send.at[i], kv_swap_recv.at[i], sibling,
        )
        for i, ref in enumerate((kx, vx))
    ]

    def swap_copies(j):
        return [
            remote(
                ref.at[core, :, cols(other, j, wide)], ref.at[core, :, cols(other, j, wide)],
                swap_send.at[i, j], swap_recv.at[i, j], sibling,
            )
            for i, ref in enumerate((qx, gx))
        ]

    def doc_copies(j, i, source_core):
        from_rows = pl.ds(pl.multiple_of(source_core * tokens, tokens), tokens)
        src, dst = ((kx, kd), (vx, vd))[i]
        return [
            remote(
                src.at[source_core, :, cols(half, j, HD)], dst.at[j, from_rows],
                doc_send.at[half, i, j], doc_recv.at[source_core, i, j], CORES + half,
            )
            for half in range(CORES)
        ]

    def term_copies(j, i, half):
        return [
            remote(
                away.at[i, j, pl.ds(keeper * tokens, tokens)], back.at[i, half, j],
                term_send.at[i, keeper, j], term_recv.at[i, half, j], keeper,
            )
            for keeper in range(CORES)
        ]

    def part_copy(j, i):
        return remote(
            part.at[i, j], acc.at[i, core, j], part_send.at[i, j], part_recv.at[i, j], sibling
        )

    def out_copy(j, i):
        ref, width = ((dq, wide), (dk, HD), (dv, HD))[i]
        view = ref.at[other, :, cols(core, j, width)]
        return remote(view, view, out_send.at[i, j], out_recv.at[i, j], sibling)

    lengths_copy = pltpu.make_async_copy(lengths_hbm, lengths_ref, lengths_sem)
    for copy in kv_own:
        copy.start()
    lengths_copy.start()
    for j in range(heads):
        for copy in own_copies(j, 1) + own_copies(j, 0):
            copy.start()

    barrier = pltpu.get_barrier_semaphore()
    for step in range(1, 2 * CORES):
        pl.semaphore_signal(
            barrier, inc=1, device_id={"sp": lax.rem(me + step, 2 * CORES)}, device_id_type=MESH
        )
    pl.semaphore_wait(barrier, 2 * CORES - 1)
    for copy in kv_own:
        copy.wait()

    @pl.when(chip == 0)
    def _():
        for j in range(heads):
            for i in range(2):
                for copy in doc_copies(j, i, core):
                    copy.start()

    for copy in kv_swap:
        copy.start()
    for j in range(heads):
        for copy in own_copies(j, 1):
            copy.wait()
        for copy in swap_copies(j):
            copy.start()

    lengths_copy.wait()
    places = chip * rows + lax.broadcasted_iota(jnp.int32, (1, rows), 1)
    doc_len = rows
    asked = places - doc_len
    start = jnp.zeros((1, rows), jnp.int32)
    end = jnp.int32(0)
    for c in range(lengths_ref.shape[0]):
        end = end + lengths_ref[c]
        start = jnp.where(end <= asked, end, start)
    first = jnp.where(asked < 0, 0, start + doc_len)
    key_places = chip * rows + lax.broadcasted_iota(jnp.int32, (rows, rows), 0)
    query_places = chip * rows + lax.broadcasted_iota(jnp.int32, (rows, rows), 1)
    seen = (key_places <= query_places) & (key_places >= first)
    bias[...] = jnp.where(seen, 0.0, MASKED)

    for copy in kv_swap:
        copy.wait()

    tiles = [(a, p) for a in range(CORES) for p in range(pairs)]

    def head_cols(j, h):
        return pl.ds(pl.multiple_of((core * heads + j) * wide + h * HD, HD), HD)

    def block(ref, j, a, p):
        return jnp.concatenate(
            [ref[a, :, head_cols(j, 2 * p)], ref[a, :, head_cols(j, 2 * p + 1)]], axis=0
        )

    def whole(ref, j, first_a):
        return jnp.concatenate(
            [block(ref, j, a, p) for a, p in tiles if a >= first_a], axis=0
        )

    def own(ref, j, a):
        return ref[: a + 1, :, cols(core, j, HD)].reshape((a + 1) * tokens, HD)

    def span(n):
        return slice(n * rows, (n + 1) * rows)

    def arrive(j):
        for copy in own_copies(j, 0) + swap_copies(j):
            copy.wait()

    def own_scores(j, low):
        for n, (a, p) in enumerate(tiles):
            seen_keys = (a + 1) * tokens
            raw = dot(own(kx, j, a), block(qx, j, a, p), 1, 1)
            mask = bias[:seen_keys, a * tokens : (a + 1) * tokens]
            probs[n, low : low + seen_keys] = raw + jnp.concatenate([mask, mask], axis=1)

    def own_grads(j, low):
        for n, (a, p) in enumerate(tiles):
            grads[n, low : low + (a + 1) * tokens] = dot(own(vx, j, a), block(gx, j, a, p), 1, 1)

    def normalize(j, low):
        for n, (a, p) in enumerate(tiles):
            extent = low + (a + 1) * tokens
            raw = probs[n, low:extent]
            if low:
                raw = jnp.concatenate([dot(kd[j], block(qx, j, a, p), 1, 1), raw], axis=0)
            peak = jnp.max(raw, axis=0, keepdims=True)
            weight = jnp.exp2((raw - peak) * (scaling * math.log2(math.e)))
            total = jnp.sum(weight, axis=0, keepdims=True)
            single = weight * (1.0 / total)
            probs[n, :extent] = single
            probs_low[:extent, span(n)] = single.astype(jnp.bfloat16)

    def differentiate(j, low):
        for n, (a, p) in enumerate(tiles):
            extent = low + (a + 1) * tokens
            single = probs[n, :extent]
            grad = grads[n, low:extent]
            if low:
                grad = jnp.concatenate([dot(vd[j], block(gx, j, a, p), 1, 1), grad], axis=0)
            delta = jnp.sum(single * grad, axis=0, keepdims=True)
            score_low[:extent, span(n)] = (single * (grad - delta)).astype(jnp.bfloat16)

    def sum_over(low_ref, ref, j, low):
        everyone = whole(ref, j, 0)
        return [
            dot(
                low_ref[low + b * tokens : low + (b + 1) * tokens, b * pairs * rows :],
                everyone[b * pairs * rows :], 1, 0,
            )
            for b in range(CORES)
        ]

    def query_grads(j, low):
        keys = own(kx, j, CORES - 1)
        if low:
            keys = jnp.concatenate([kd[j], keys], axis=0)
        keys_flat = flip(keys).astype(jnp.bfloat16)
        for n, (a, p) in enumerate(tiles):
            extent = low + (a + 1) * tokens
            flat = dot(keys_flat[:, :extent], score_low[:extent, span(n)], 1, 0) * scaling
            for h in range(2):
                dq[a, :, head_cols(j, 2 * p + h)] = jnp.transpose(
                    flat[:, h * tokens : (h + 1) * tokens]
                ).astype(jnp.bfloat16)

    @pl.when(chip == 0)
    def _():
        def keep(i, j, low, high):
            acc[i, core, j] = jnp.where(core == 0, low, high)
            part[i, j] = jnp.where(core == 0, high, low)
            part_copy(j, i).start()

        def step(j, carry):
            arrive(j)
            own_scores(j, 0)
            own_grads(j, 0)
            normalize(j, 0)
            low, high = sum_over(probs_low, gx, j, 0)
            keep(1, j, low, high)
            differentiate(j, 0)
            low, high = sum_over(score_low, qx, j, 0)
            keep(0, j, low * scaling, high * scaling)
            query_grads(j, 0)
            out_copy(j, 0).start()
            return carry

        lax.fori_loop(0, heads, step, 0)

        def finish(j, carry):
            for i in (1, 0):
                part_copy(j, i).wait()
                for half in range(CORES):
                    term_copies(j, i, half)[0].wait_recv()
                    total = acc[i, half, j] + back[i, half, j].astype(jnp.float32)
                    (dk, dv)[i][core, :, cols(half, j, HD)] = total.astype(jnp.bfloat16)
            return carry

        lax.fori_loop(0, heads, finish, 0)
        for j in range(heads):
            for i in range(2):
                for copy in doc_copies(j, i, core):
                    copy.wait_send()
            out_copy(j, 0).wait()

    @pl.when(chip == 1)
    def _():
        def step(j, carry):
            arrive(j)
            own_scores(j, rows)
            for source_core in range(CORES):
                doc_copies(j, 0, source_core)[0].wait_recv()
            normalize(j, rows)
            away[1, j] = dot(probs_low[:rows], whole(gx, j, 0), 1, 0).astype(jnp.bfloat16)
            for copy in term_copies(j, 1, core):
                copy.start()
            own_grads(j, rows)
            for a, total in enumerate(sum_over(probs_low, gx, j, rows)):
                dv[a, :, cols(core, j, HD)] = total.astype(jnp.bfloat16)
            for source_core in range(CORES):
                doc_copies(j, 1, source_core)[0].wait_recv()
            differentiate(j, rows)
            away[0, j] = (dot(score_low[:rows], whole(qx, j, 0), 1, 0) * scaling).astype(
                jnp.bfloat16
            )
            for copy in term_copies(j, 0, core):
                copy.start()
            for a, total in enumerate(sum_over(score_low, qx, j, rows)):
                dk[a, :, cols(core, j, HD)] = (total * scaling).astype(jnp.bfloat16)
            query_grads(j, rows)
            for i in range(3):
                out_copy(j, i).start()
            return carry

        lax.fori_loop(0, heads, step, 0)
        for j in range(heads):
            for i in range(2):
                for copy in term_copies(j, i, core):
                    copy.wait_send()
            for i in range(3):
                out_copy(j, i).wait()


def pair_kernel(tokens, heads, group, *refs):
    sems = lambda *shape: pltpu.SemaphoreType.DMA(shape)
    pl.run_scoped(
        lambda *scoped: pair_body(tokens, heads, group, *refs, *scoped),
        pltpu.SemaphoreType.DMA,
        sems(2),
        sems(2, CORES, heads),
        sems(2),
        sems(2),
        sems(2, heads),
        sems(2, heads),
        sems(CORES, 2, heads),
        sems(CORES, 2, heads),
        sems(2, CORES, heads),
        sems(2, CORES, heads),
        sems(2, heads),
        sems(2, heads),
        sems(3, heads),
        sems(3, heads),
    )


def publish_kernel(dq_in, dk_in, dv_in, dq_out, dk_out, dv_out, sem):
    core = lax.rem(lax.axis_index("sp"), CORES)
    copies = [
        pltpu.make_async_copy(src.at[core], dst, sem.at[i])
        for i, (src, dst) in enumerate(((dq_in, dq_out), (dk_in, dk_out), (dv_in, dv_out)))
    ]
    for copy in copies:
        copy.start()
    for copy in copies:
        copy.wait()


def on_pairs(query_rows, key_rows, value_rows, out_grad, question_lengths):
    tokens = query_rows.shape[0]
    heads = KVH // CORES
    group = QH // KVH
    rows = tokens * CORES
    low, wide = jnp.bfloat16, jnp.float32
    vmem, sems = pltpu.VMEM, lambda *shape: pltpu.SemaphoreType.DMA(shape)
    anywhere = pl.BlockSpec(memory_space=pl.ANY)
    tiles = group * CORES // 2
    grads = pl.pallas_call(
        partial(pair_kernel, tokens, heads, group),
        out_shape=tuple(
            pltpu.VMEM((CORES,) + array.shape, low) for array in (query_rows, key_rows, value_rows)
        ),
        in_specs=[anywhere] * 5,
        out_specs=(pl.BlockSpec(memory_space=pltpu.VMEM),) * 3,
        scratch_shapes=[
            vmem((CORES,) + query_rows.shape, low),
            vmem((CORES,) + query_rows.shape, low),
            vmem((CORES,) + key_rows.shape, low),
            vmem((CORES,) + key_rows.shape, low),
            vmem((heads, rows, HD), low),
            vmem((heads, rows, HD), low),
            vmem((rows, rows), wide),
            vmem((tiles, 2 * rows, rows), wide),
            vmem((tiles, 2 * rows, rows), wide),
            vmem((2 * rows, tiles * rows), low),
            vmem((2 * rows, tiles * rows), low),
            vmem((2, CORES, heads, tokens, HD), wide),
            vmem((2, heads, tokens, HD), wide),
            vmem((2, heads, rows, HD), low),
            vmem((2, CORES, heads, tokens, HD), low),
            pltpu.SMEM(question_lengths.shape, jnp.int32),
        ],
        compiler_params=pltpu.CompilerParams(
            collective_id=0, has_side_effects=True,
        ),
    )(question_lengths, query_rows, out_grad, key_rows, value_rows)
    return pl.pallas_call(
        publish_kernel,
        out_shape=tuple(
            jax.ShapeDtypeStruct(array.shape, low) for array in (query_rows, key_rows, value_rows)
        ),
        in_specs=[anywhere] * 3,
        out_specs=(anywhere,) * 3,
        scratch_shapes=[sems(3)],
        compiler_params=pltpu.CompilerParams(has_side_effects=True, vmem_limit_bytes=1024 * 1024),
    )(*grads)


def solution(mesh):
    body = on_pairs if mesh.shape["sp"] == 2 * CORES else on_device
    return jax.shard_map(
        body,
        mesh=mesh,
        in_specs=(
            P(("grp", "sp"), None),
            P(("grp", "sp"), None),
            P(("grp", "sp"), None),
            P(("grp", "sp"), None),
            P("grp"),
        ),
        out_specs=(P(("grp", "sp"), None), P(("grp", "sp"), None), P(("grp", "sp"), None)),
        check_vma=False,
    )
```

```python
from functools import partial
from functools import reduce
import math

import jax
import jax.numpy as jnp
from jax import lax
from jax.experimental import pallas as pl
from jax.experimental.pallas import tpu as pltpu
from jax.sharding import PartitionSpec as P

HD = 128
QH = 32
KVH = 8


MASKED = -1e30


def widen(rows, copies):
    tokens = rows.shape[0]
    shaped = rows.reshape(tokens, KVH, 1, HD)
    return jnp.broadcast_to(shaped, (tokens, KVH, copies, HD)).reshape(tokens, KVH * copies * HD)


def segment_ids(question_lengths, length, doc_len):
    ends = jnp.cumsum(question_lengths)
    places = jnp.arange(length, dtype=jnp.int32)
    inside = jnp.sum((ends[None, :] <= (places - doc_len)[:, None]).astype(jnp.int32), axis=1)
    return jnp.where(places < doc_len, -1, inside)


def make_scores(query_block, key_block, visible, scaling):
    raw = (
        jnp.einsum("bkgd,skd->kgbs", query_block, key_block, preferred_element_type=jnp.float32)
        * scaling
    )
    return jnp.where(visible[None, None], raw, MASKED)


def weighted_values(probs_b, value_block):
    return jnp.einsum("kgbs,skd->bkgd", probs_b, value_block, preferred_element_type=jnp.float32)


def backward_block(probs, probs_b, delta, grad_block, query_block, key_block, value_block, scaling):
    value_part = jnp.einsum(
        "kgbs,bkgd->skd", probs_b, grad_block, preferred_element_type=jnp.float32
    )
    prob_grad = jnp.einsum(
        "bkgd,skd->kgbs", grad_block, value_block, preferred_element_type=jnp.float32
    )
    score_grad = (probs * (prob_grad - delta[..., None])).astype(jnp.bfloat16)
    query_part = jnp.einsum(
        "kgbs,skd->bkgd", score_grad, key_block, preferred_element_type=jnp.float32
    )
    key_part = (
        jnp.einsum("kgbs,bkgd->skd", score_grad, query_block, preferred_element_type=jnp.float32)
        * scaling
    )
    return (query_part, key_part, value_part)


def on_device(query_rows, key_rows, value_rows, out_grad, question_lengths):
    devices = lax.axis_size("sp")
    tokens = query_rows.shape[0]
    length = tokens * devices
    doc_len = length // 2
    block_len = min(512, length)
    block_count = length // block_len
    scaling = 1.0 / math.sqrt(HD)
    copies = max(KVH, devices) // KVH
    keys_local, values_local = (
        lax.all_to_all(widen(key_rows, copies), "sp", split_axis=1, concat_axis=0, tiled=True),
        lax.all_to_all(widen(value_rows, copies), "sp", split_axis=1, concat_axis=0, tiled=True),
    )
    queries_local, grads_local = (
        lax.all_to_all(query_rows, "sp", split_axis=1, concat_axis=0, tiled=True),
        lax.all_to_all(out_grad, "sp", split_axis=1, concat_axis=0, tiled=True),
    )
    key_heads = KVH * copies // devices
    per_group = QH // devices // key_heads
    queries = queries_local.reshape(length, key_heads, per_group, HD)
    grads = grads_local.reshape(length, key_heads, per_group, HD)
    keys = keys_local.reshape(length, key_heads, HD)
    values = values_local.reshape(length, key_heads, HD)
    segment = segment_ids(question_lengths, length, doc_len)
    places = jnp.arange(length, dtype=jnp.int32)
    query_shape = (block_len, key_heads, per_group, HD)
    key_shape = (block_len, key_heads, HD)
    key_sums = [jnp.zeros(key_shape, jnp.float32)] * block_count
    value_sums = [jnp.zeros(key_shape, jnp.float32)] * block_count
    query_parts = []
    for row_block in range(block_count):
        row_start = row_block * block_len
        query_block = queries[row_start : row_start + block_len]
        grad_block = grads[row_start : row_start + block_len]
        row_places = places[row_start : row_start + block_len]
        row_segment = segment[row_start : row_start + block_len]
        needs = []
        scores = []
        for col_block in range(row_block + 1):
            col_start = col_block * block_len
            col_places = places[col_start : col_start + block_len]
            col_segment = segment[col_start : col_start + block_len]
            visible = (col_places[None, :] <= row_places[:, None]) & (
                (col_places[None, :] < doc_len) | (col_segment[None, :] == row_segment[:, None])
            )
            needed = True
            needs.append(needed)
            scores.append(
                make_scores(query_block, keys[col_start : col_start + block_len], visible, scaling)
            )
        peak = reduce(jnp.maximum, [jnp.max(score, axis=3) for score in scores])
        total = reduce(
            jnp.add, [jnp.sum(jnp.exp(score - peak[..., None]), axis=3) for score in scores]
        )
        log_total = peak + jnp.log(total)
        probs = [jnp.exp(score - log_total[..., None]) for score in scores]
        probs_low = [single.astype(jnp.bfloat16) for single in probs]
        output = jnp.zeros(query_shape, jnp.float32)
        for col_block in range(row_block + 1):
            col_start = col_block * block_len
            output = output + weighted_values(
                probs_low[col_block], values[col_start : col_start + block_len]
            )
        output_low = output.astype(jnp.bfloat16)
        delta = jnp.einsum(
            "bkgd,bkgd->kgb", grad_block, output_low, preferred_element_type=jnp.float32
        )
        query_sum = jnp.zeros(query_shape, jnp.float32)
        for col_block in range(row_block + 1):
            col_start = col_block * block_len
            action = partial(
                backward_block,
                probs[col_block],
                probs_low[col_block],
                delta,
                grad_block,
                query_block,
                keys[col_start : col_start + block_len],
                values[col_start : col_start + block_len],
                scaling,
            )
            query_part, key_part, value_part = action()
            query_sum = query_sum + query_part
            key_sums[col_block] = key_sums[col_block] + key_part
            value_sums[col_block] = value_sums[col_block] + value_part
        query_parts.append((query_sum * scaling).astype(jnp.bfloat16))
    query_local = jnp.concatenate(query_parts, axis=0).reshape(length, key_heads * per_group * HD)
    key_local = jnp.concatenate(key_sums, axis=0).reshape(length, key_heads * HD)
    value_local = jnp.concatenate(value_sums, axis=0).reshape(length, key_heads * HD)
    query_grad = lax.all_to_all(query_local, "sp", split_axis=0, concat_axis=1, tiled=True)
    key_back, value_back = (
        lax.all_to_all(key_local, "sp", split_axis=0, concat_axis=1, tiled=True),
        lax.all_to_all(value_local, "sp", split_axis=0, concat_axis=1, tiled=True),
    )
    key_grad = (
        jnp.sum(key_back.reshape(tokens, KVH, copies, HD), axis=2)
        .reshape(tokens, KVH * HD)
        .astype(jnp.bfloat16)
    )
    value_grad = (
        jnp.sum(value_back.reshape(tokens, KVH, copies, HD), axis=2)
        .reshape(tokens, KVH * HD)
        .astype(jnp.bfloat16)
    )
    return (query_grad, key_grad, value_grad)


MESH = pl.DeviceIdType.MESH
CORES = 2
CHUNK = 32


def dot(left, right, left_dim, right_dim):
    return lax.dot_general(
        left, right, (((left_dim,), (right_dim,)), ((), ())), preferred_element_type=jnp.float32
    )


def flip(tile):
    return jnp.transpose(tile.astype(jnp.float32))


def pair_body(
    tokens, heads, group, lengths_hbm, q_hbm, g_hbm, k_hbm, v_hbm, dq, dk, dv,
    qx, gx, kx, vx, kd, vd, bias, probs, outs, probs_low, score_low, flat, turned, inverses, acc, part, away, back,
    lengths_ref, lengths_sem, kv_sem, own_sem, kv_swap_send, kv_swap_recv, swap_send, swap_recv,
    doc_send, doc_recv, term_send, term_recv, part_send, part_recv, out_send, out_recv,
):
    me = lax.axis_index("sp")
    chip = me // CORES
    core = lax.rem(me, CORES)
    other = 1 - core
    sibling = chip * CORES + other
    rows = tokens * CORES
    wide = group * HD
    pairs = group // 2
    scaling = 1.0 / math.sqrt(HD)

    def cols(half, j, width):
        return pl.ds(pl.multiple_of((half * heads + j) * width, width), width)

    def remote(src, dst, send, recv, device):
        return pltpu.make_async_remote_copy(
            src_ref=src, dst_ref=dst, send_sem=send, recv_sem=recv,
            device_id={"sp": device}, device_id_type=MESH,
        )

    kv_own = [
        pltpu.make_async_copy(src, dst.at[core], kv_sem.at[i])
        for i, (src, dst) in enumerate(((k_hbm, kx), (v_hbm, vx)))
    ]

    def own_copies(j, which):
        half = (core, other)[which]
        return [
            pltpu.make_async_copy(
                src.at[:, cols(half, j, wide)], dst.at[core, :, cols(half, j, wide)],
                own_sem.at[i, which, j],
            )
            for i, (src, dst) in enumerate(((q_hbm, qx), (g_hbm, gx)))
        ]

    kv_half = pl.ds(pl.multiple_of(other * heads * HD, heads * HD), heads * HD)
    kv_swap = [
        remote(
            ref.at[core, :, kv_half], ref.at[core, :, kv_half],
            kv_swap_send.at[i], kv_swap_recv.at[i], sibling,
        )
        for i, ref in enumerate((kx, vx))
    ]

    def swap_copies(j):
        return [
            remote(
                ref.at[core, :, cols(other, j, wide)], ref.at[core, :, cols(other, j, wide)],
                swap_send.at[i, j], swap_recv.at[i, j], sibling,
            )
            for i, ref in enumerate((qx, gx))
        ]

    def doc_copies(j, i, source_core):
        from_rows = pl.ds(pl.multiple_of(source_core * tokens, tokens), tokens)
        src, dst = ((kx, kd), (vx, vd))[i]
        return [
            remote(
                src.at[source_core, :, cols(half, j, HD)], dst.at[j, from_rows],
                doc_send.at[half, i, j], doc_recv.at[source_core, i, j], CORES + half,
            )
            for half in range(CORES)
        ]

    def term_copies(j, i, half):
        return [
            remote(
                away.at[i, j, pl.ds(keeper * tokens, tokens)], back.at[i, half, j],
                term_send.at[i, keeper, j], term_recv.at[i, half, j], keeper,
            )
            for keeper in range(CORES)
        ]

    def part_copy(j, i):
        return remote(
            part.at[i, j], acc.at[i, core, j], part_send.at[i, j], part_recv.at[i, j], sibling
        )

    def out_copy(j, i):
        ref, width = ((dq, wide), (dk, HD), (dv, HD))[i]
        view = ref.at[other, :, cols(core, j, width)]
        return remote(view, view, out_send.at[i, j], out_recv.at[i, j], sibling)

    lengths_copy = pltpu.make_async_copy(lengths_hbm, lengths_ref, lengths_sem)
    for copy in kv_own:
        copy.start()
    lengths_copy.start()
    for j in range(heads):
        for copy in own_copies(j, 1) + own_copies(j, 0):
            copy.start()

    barrier = pltpu.get_barrier_semaphore()
    for step in range(1, 2 * CORES):
        pl.semaphore_signal(
            barrier, inc=1, device_id={"sp": lax.rem(me + step, 2 * CORES)}, device_id_type=MESH
        )
    pl.semaphore_wait(barrier, 2 * CORES - 1)
    for copy in kv_own:
        copy.wait()

    @pl.when(chip == 0)
    def _():
        for j in range(heads):
            for i in range(2):
                for copy in doc_copies(j, i, core):
                    copy.start()

    for copy in kv_swap:
        copy.start()
    for j in range(heads):
        for copy in own_copies(j, 1):
            copy.wait()
        for copy in swap_copies(j):
            copy.start()

    lengths_copy.wait()
    places = chip * rows + lax.broadcasted_iota(jnp.int32, (1, rows), 1)
    doc_len = rows
    asked = places - doc_len
    start = jnp.zeros((1, rows), jnp.int32)
    end = jnp.int32(0)
    for c in range(lengths_ref.shape[0]):
        end = end + lengths_ref[c]
        start = jnp.where(end <= asked, end, start)
    first = jnp.where(asked < 0, 0, start + doc_len)
    key_places = chip * rows + lax.broadcasted_iota(jnp.int32, (rows, rows), 0)
    query_places = chip * rows + lax.broadcasted_iota(jnp.int32, (rows, rows), 1)
    seen = (key_places <= query_places) & (key_places >= first)
    bias[...] = jnp.where(seen, 0.0, MASKED)

    for copy in kv_swap:
        copy.wait()

    tiles = [(a, p) for a in range(CORES) for p in range(pairs)]

    def head_cols(j, h):
        return pl.ds(pl.multiple_of((core * heads + j) * wide + h * HD, HD), HD)

    def block(ref, j, a, p):
        return jnp.concatenate(
            [ref[a, :, head_cols(j, 2 * p)], ref[a, :, head_cols(j, 2 * p + 1)]], axis=0
        )

    def whole(ref, j, first_a):
        return jnp.concatenate(
            [block(ref, j, a, p) for a, p in tiles if a >= first_a], axis=0
        )

    def own(ref, j, a):
        return ref[: a + 1, :, cols(core, j, HD)].reshape((a + 1) * tokens, HD)

    def span(n):
        return slice(n * rows, (n + 1) * rows)

    def arrive(j):
        for copy in own_copies(j, 0) + swap_copies(j):
            copy.wait()

    def own_scores(j, low):
        for n, (a, p) in enumerate(tiles):
            seen_keys = (a + 1) * tokens
            raw = dot(own(kx, j, a), block(qx, j, a, p), 1, 1)
            mask = bias[:seen_keys, a * tokens : (a + 1) * tokens]
            probs[n, low : low + seen_keys] = raw + jnp.concatenate([mask, mask], axis=1)
            flat[:, span(n)] = flip(block(gx, j, a, p)).astype(jnp.bfloat16)
        turned[:, low : low + rows] = flip(own(vx, j, CORES - 1)).astype(jnp.bfloat16)

    def own_outputs(j, low):
        for n, (a, p) in enumerate(tiles):
            extent = low + (a + 1) * tokens
            outs[n] = dot(turned[:, low:extent], probs_low[low:extent, span(n)], 1, 0)

    def fold(chunk, op):
        return op(chunk.reshape(chunk.shape[0] // 8, 8, chunk.shape[1]), axis=0)

    def normalize(j, low):
        if low:
            for n, (a, p) in enumerate(tiles):
                probs[n, :low] = dot(kd[j], block(qx, j, a, p), 1, 1)
        for n, (a, p) in enumerate(tiles):
            extent = low + (a + 1) * tokens
            peak = None
            for r in range(0, extent, CHUNK):
                high = fold(probs[n, r : r + CHUNK], jnp.max)
                peak = high if peak is None else jnp.maximum(peak, high)
            peak = jnp.max(peak, axis=0, keepdims=True)
            total = None
            for r in range(0, extent, CHUNK):
                weight = jnp.exp2((probs[n, r : r + CHUNK] - peak) * (scaling * math.log2(math.e)))
                probs_low[r : r + CHUNK, span(n)] = weight.astype(jnp.bfloat16)
                part_total = fold(weight, jnp.sum)
                total = part_total if total is None else total + part_total
            inverse = 1.0 / jnp.sum(total, axis=0, keepdims=True)
            inverses[n] = jnp.broadcast_to(inverse, (8, rows))
            flat[:, span(n)] = (flat[:, span(n)].astype(jnp.float32) * inverse).astype(jnp.bfloat16)

    def deltas(j, low):
        if low:
            turned[:, :low] = flip(vd[j]).astype(jnp.bfloat16)
        for n, (a, p) in enumerate(tiles):
            output = outs[n]
            if low:
                output = output + dot(turned[:, :low], probs_low[:low, span(n)], 1, 0)
            delta = jnp.sum(output * flat[:, span(n)].astype(jnp.float32), axis=0, keepdims=True)
            inverses[n] = inverses[n] * delta

    def differentiate(j, start, keys_of):
        for n, (a, p) in enumerate(tiles):
            values = keys_of(a)
            here = slice(start, start + values.shape[0])
            grad = dot(values, flat[:, span(n)], 1, 0)
            single = probs_low[here, span(n)].astype(jnp.float32)
            score_low[here, span(n)] = (single * (grad - inverses[n, :1])).astype(jnp.bfloat16)

    def doc_sum(low_ref, other, j):
        if low_ref is probs_low:
            return dot(low_ref[:rows], flat[...], 1, 1)
        return dot(low_ref[:rows], whole(other, j, 0), 1, 0)

    def sum_over(low_ref, other, j, low):
        sums = []
        for b in range(CORES):
            left = low_ref[low + b * tokens : low + (b + 1) * tokens, b * pairs * rows :]
            if low_ref is probs_low:
                sums.append(dot(left, flat[:, b * pairs * rows :], 1, 1))
            else:
                sums.append(dot(left, whole(other, j, b), 1, 0))
        return sums

    def query_grads(j, low):
        keys = own(kx, j, CORES - 1)
        if low:
            keys = jnp.concatenate([kd[j], keys], axis=0)
        keys_flat = flip(keys).astype(jnp.bfloat16)
        for n, (a, p) in enumerate(tiles):
            extent = low + (a + 1) * tokens
            result = dot(keys_flat[:, :extent], score_low[:extent, span(n)], 1, 0) * scaling
            for h in range(2):
                dq[a, :, head_cols(j, 2 * p + h)] = jnp.transpose(
                    result[:, h * tokens : (h + 1) * tokens]
                ).astype(jnp.bfloat16)

    @pl.when(chip == 0)
    def _():
        def keep(i, j, low, high):
            acc[i, core, j] = jnp.where(core == 0, low, high)
            part[i, j] = jnp.where(core == 0, high, low)
            part_copy(j, i).start()

        def step(j, carry):
            arrive(j)
            own_scores(j, 0)
            normalize(j, 0)
            own_outputs(j, 0)
            low, high = sum_over(probs_low, gx, j, 0)
            keep(1, j, low, high)
            deltas(j, 0)
            differentiate(j, 0, lambda a: own(vx, j, a))
            low, high = sum_over(score_low, qx, j, 0)
            keep(0, j, low * scaling, high * scaling)
            query_grads(j, 0)
            out_copy(j, 0).start()
            return carry

        lax.fori_loop(0, heads, step, 0)

        def finish(j, carry):
            for i in (1, 0):
                part_copy(j, i).wait()
                for half in range(CORES):
                    term_copies(j, i, half)[0].wait_recv()
                    total = acc[i, half, j] + back[i, half, j].astype(jnp.float32)
                    (dk, dv)[i][core, :, cols(half, j, HD)] = total.astype(jnp.bfloat16)
            return carry

        lax.fori_loop(0, heads, finish, 0)
        for j in range(heads):
            for i in range(2):
                for copy in doc_copies(j, i, core):
                    copy.wait_send()
            out_copy(j, 0).wait()

    @pl.when(chip == 1)
    def _():
        def step(j, carry):
            arrive(j)
            own_scores(j, rows)
            for source_core in range(CORES):
                doc_copies(j, 0, source_core)[0].wait_recv()
            normalize(j, rows)
            away[1, j] = doc_sum(probs_low, gx, j).astype(jnp.bfloat16)
            for copy in term_copies(j, 1, core):
                copy.start()
            own_outputs(j, rows)
            for a, total in enumerate(sum_over(probs_low, gx, j, rows)):
                dv[a, :, cols(core, j, HD)] = total.astype(jnp.bfloat16)
            for source_core in range(CORES):
                doc_copies(j, 1, source_core)[0].wait_recv()
            deltas(j, rows)
            differentiate(j, 0, lambda a: vd[j])
            away[0, j] = (doc_sum(score_low, qx, j) * scaling).astype(
                jnp.bfloat16
            )
            for copy in term_copies(j, 0, core):
                copy.start()
            differentiate(j, rows, lambda a: own(vx, j, a))
            for a, total in enumerate(sum_over(score_low, qx, j, rows)):
                dk[a, :, cols(core, j, HD)] = (total * scaling).astype(jnp.bfloat16)
            query_grads(j, rows)
            for i in range(3):
                out_copy(j, i).start()
            return carry

        lax.fori_loop(0, heads, step, 0)
        for j in range(heads):
            for i in range(2):
                for copy in term_copies(j, i, core):
                    copy.wait_send()
            for i in range(3):
                out_copy(j, i).wait()


def pair_kernel(tokens, heads, group, *refs):
    sems = lambda *shape: pltpu.SemaphoreType.DMA(shape)
    pl.run_scoped(
        lambda *scoped: pair_body(tokens, heads, group, *refs, *scoped),
        pltpu.SemaphoreType.DMA,
        sems(2),
        sems(2, CORES, heads),
        sems(2),
        sems(2),
        sems(2, heads),
        sems(2, heads),
        sems(CORES, 2, heads),
        sems(CORES, 2, heads),
        sems(2, CORES, heads),
        sems(2, CORES, heads),
        sems(2, heads),
        sems(2, heads),
        sems(3, heads),
        sems(3, heads),
    )


def publish_kernel(dq_in, dk_in, dv_in, dq_out, dk_out, dv_out, sem):
    core = lax.rem(lax.axis_index("sp"), CORES)
    copies = [
        pltpu.make_async_copy(src.at[core], dst, sem.at[i])
        for i, (src, dst) in enumerate(((dq_in, dq_out), (dk_in, dk_out), (dv_in, dv_out)))
    ]
    for copy in copies:
        copy.start()
    for copy in copies:
        copy.wait()


def on_pairs(query_rows, key_rows, value_rows, out_grad, question_lengths):
    tokens = query_rows.shape[0]
    heads = KVH // CORES
    group = QH // KVH
    rows = tokens * CORES
    low, wide = jnp.bfloat16, jnp.float32
    vmem, sems = pltpu.VMEM, lambda *shape: pltpu.SemaphoreType.DMA(shape)
    anywhere = pl.BlockSpec(memory_space=pl.ANY)
    tiles = group * CORES // 2
    grads = pl.pallas_call(
        partial(pair_kernel, tokens, heads, group),
        out_shape=tuple(
            pltpu.VMEM((CORES,) + array.shape, low) for array in (query_rows, key_rows, value_rows)
        ),
        in_specs=[anywhere] * 5,
        out_specs=(pl.BlockSpec(memory_space=pltpu.VMEM),) * 3,
        scratch_shapes=[
            vmem((CORES,) + query_rows.shape, low),
            vmem((CORES,) + query_rows.shape, low),
            vmem((CORES,) + key_rows.shape, low),
            vmem((CORES,) + key_rows.shape, low),
            vmem((heads, rows, HD), low),
            vmem((heads, rows, HD), low),
            vmem((rows, rows), wide),
            vmem((tiles, 2 * rows, rows), wide),
            vmem((tiles, HD, rows), wide),
            vmem((2 * rows, tiles * rows), low),
            vmem((2 * rows, tiles * rows), low),
            vmem((HD, tiles * rows), low),
            vmem((HD, 2 * rows), low),
            vmem((tiles, 8, rows), wide),
            vmem((2, CORES, heads, tokens, HD), wide),
            vmem((2, heads, tokens, HD), wide),
            vmem((2, heads, rows, HD), low),
            vmem((2, CORES, heads, tokens, HD), low),
            pltpu.SMEM(question_lengths.shape, jnp.int32),
        ],
        compiler_params=pltpu.CompilerParams(
            collective_id=0, has_side_effects=True,
        ),
    )(question_lengths, query_rows, out_grad, key_rows, value_rows)
    return pl.pallas_call(
        publish_kernel,
        out_shape=tuple(
            jax.ShapeDtypeStruct(array.shape, low) for array in (query_rows, key_rows, value_rows)
        ),
        in_specs=[anywhere] * 3,
        out_specs=(anywhere,) * 3,
        scratch_shapes=[sems(3)],
        compiler_params=pltpu.CompilerParams(has_side_effects=True, vmem_limit_bytes=1024 * 1024),
    )(*grads)


def solution(mesh):
    body = on_pairs if mesh.shape["sp"] == 2 * CORES else on_device
    return jax.shard_map(
        body,
        mesh=mesh,
        in_specs=(
            P(("grp", "sp"), None),
            P(("grp", "sp"), None),
            P(("grp", "sp"), None),
            P(("grp", "sp"), None),
            P("grp"),
        ),
        out_specs=(P(("grp", "sp"), None), P(("grp", "sp"), None), P(("grp", "sp"), None)),
        check_vma=False,
    )
```

```python
from functools import partial
from functools import reduce
import math

import jax
import jax.numpy as jnp
from jax import lax
from jax.experimental import pallas as pl
from jax.experimental.pallas import tpu as pltpu
from jax.sharding import PartitionSpec as P

HD = 128
QH = 32
KVH = 8


MASKED = -1e30


def widen(rows, copies):
    tokens = rows.shape[0]
    shaped = rows.reshape(tokens, KVH, 1, HD)
    return jnp.broadcast_to(shaped, (tokens, KVH, copies, HD)).reshape(tokens, KVH * copies * HD)


def segment_ids(question_lengths, length, doc_len):
    ends = jnp.cumsum(question_lengths)
    places = jnp.arange(length, dtype=jnp.int32)
    inside = jnp.sum((ends[None, :] <= (places - doc_len)[:, None]).astype(jnp.int32), axis=1)
    return jnp.where(places < doc_len, -1, inside)


def make_scores(query_block, key_block, visible, scaling):
    raw = (
        jnp.einsum("bkgd,skd->kgbs", query_block, key_block, preferred_element_type=jnp.float32)
        * scaling
    )
    return jnp.where(visible[None, None], raw, MASKED)


def weighted_values(probs_b, value_block):
    return jnp.einsum("kgbs,skd->bkgd", probs_b, value_block, preferred_element_type=jnp.float32)


def backward_block(probs, probs_b, delta, grad_block, query_block, key_block, value_block, scaling):
    value_part = jnp.einsum(
        "kgbs,bkgd->skd", probs_b, grad_block, preferred_element_type=jnp.float32
    )
    prob_grad = jnp.einsum(
        "bkgd,skd->kgbs", grad_block, value_block, preferred_element_type=jnp.float32
    )
    score_grad = (probs * (prob_grad - delta[..., None])).astype(jnp.bfloat16)
    query_part = jnp.einsum(
        "kgbs,skd->bkgd", score_grad, key_block, preferred_element_type=jnp.float32
    )
    key_part = (
        jnp.einsum("kgbs,bkgd->skd", score_grad, query_block, preferred_element_type=jnp.float32)
        * scaling
    )
    return (query_part, key_part, value_part)


def on_device(query_rows, key_rows, value_rows, out_grad, question_lengths):
    devices = lax.axis_size("sp")
    tokens = query_rows.shape[0]
    length = tokens * devices
    doc_len = length // 2
    block_len = min(512, length)
    block_count = length // block_len
    scaling = 1.0 / math.sqrt(HD)
    copies = max(KVH, devices) // KVH
    keys_local, values_local = (
        lax.all_to_all(widen(key_rows, copies), "sp", split_axis=1, concat_axis=0, tiled=True),
        lax.all_to_all(widen(value_rows, copies), "sp", split_axis=1, concat_axis=0, tiled=True),
    )
    queries_local, grads_local = (
        lax.all_to_all(query_rows, "sp", split_axis=1, concat_axis=0, tiled=True),
        lax.all_to_all(out_grad, "sp", split_axis=1, concat_axis=0, tiled=True),
    )
    key_heads = KVH * copies // devices
    per_group = QH // devices // key_heads
    queries = queries_local.reshape(length, key_heads, per_group, HD)
    grads = grads_local.reshape(length, key_heads, per_group, HD)
    keys = keys_local.reshape(length, key_heads, HD)
    values = values_local.reshape(length, key_heads, HD)
    segment = segment_ids(question_lengths, length, doc_len)
    places = jnp.arange(length, dtype=jnp.int32)
    query_shape = (block_len, key_heads, per_group, HD)
    key_shape = (block_len, key_heads, HD)
    key_sums = [jnp.zeros(key_shape, jnp.float32)] * block_count
    value_sums = [jnp.zeros(key_shape, jnp.float32)] * block_count
    query_parts = []
    for row_block in range(block_count):
        row_start = row_block * block_len
        query_block = queries[row_start : row_start + block_len]
        grad_block = grads[row_start : row_start + block_len]
        row_places = places[row_start : row_start + block_len]
        row_segment = segment[row_start : row_start + block_len]
        needs = []
        scores = []
        for col_block in range(row_block + 1):
            col_start = col_block * block_len
            col_places = places[col_start : col_start + block_len]
            col_segment = segment[col_start : col_start + block_len]
            visible = (col_places[None, :] <= row_places[:, None]) & (
                (col_places[None, :] < doc_len) | (col_segment[None, :] == row_segment[:, None])
            )
            needed = True
            needs.append(needed)
            scores.append(
                make_scores(query_block, keys[col_start : col_start + block_len], visible, scaling)
            )
        peak = reduce(jnp.maximum, [jnp.max(score, axis=3) for score in scores])
        total = reduce(
            jnp.add, [jnp.sum(jnp.exp(score - peak[..., None]), axis=3) for score in scores]
        )
        log_total = peak + jnp.log(total)
        probs = [jnp.exp(score - log_total[..., None]) for score in scores]
        probs_low = [single.astype(jnp.bfloat16) for single in probs]
        output = jnp.zeros(query_shape, jnp.float32)
        for col_block in range(row_block + 1):
            col_start = col_block * block_len
            output = output + weighted_values(
                probs_low[col_block], values[col_start : col_start + block_len]
            )
        output_low = output.astype(jnp.bfloat16)
        delta = jnp.einsum(
            "bkgd,bkgd->kgb", grad_block, output_low, preferred_element_type=jnp.float32
        )
        query_sum = jnp.zeros(query_shape, jnp.float32)
        for col_block in range(row_block + 1):
            col_start = col_block * block_len
            action = partial(
                backward_block,
                probs[col_block],
                probs_low[col_block],
                delta,
                grad_block,
                query_block,
                keys[col_start : col_start + block_len],
                values[col_start : col_start + block_len],
                scaling,
            )
            query_part, key_part, value_part = action()
            query_sum = query_sum + query_part
            key_sums[col_block] = key_sums[col_block] + key_part
            value_sums[col_block] = value_sums[col_block] + value_part
        query_parts.append((query_sum * scaling).astype(jnp.bfloat16))
    query_local = jnp.concatenate(query_parts, axis=0).reshape(length, key_heads * per_group * HD)
    key_local = jnp.concatenate(key_sums, axis=0).reshape(length, key_heads * HD)
    value_local = jnp.concatenate(value_sums, axis=0).reshape(length, key_heads * HD)
    query_grad = lax.all_to_all(query_local, "sp", split_axis=0, concat_axis=1, tiled=True)
    key_back, value_back = (
        lax.all_to_all(key_local, "sp", split_axis=0, concat_axis=1, tiled=True),
        lax.all_to_all(value_local, "sp", split_axis=0, concat_axis=1, tiled=True),
    )
    key_grad = (
        jnp.sum(key_back.reshape(tokens, KVH, copies, HD), axis=2)
        .reshape(tokens, KVH * HD)
        .astype(jnp.bfloat16)
    )
    value_grad = (
        jnp.sum(value_back.reshape(tokens, KVH, copies, HD), axis=2)
        .reshape(tokens, KVH * HD)
        .astype(jnp.bfloat16)
    )
    return (query_grad, key_grad, value_grad)


MESH = pl.DeviceIdType.MESH
CORES = 2
CHUNK = 32
WINDOW = 4


def dot(left, right, left_dim, right_dim):
    return lax.dot_general(
        left, right, (((left_dim,), (right_dim,)), ((), ())), preferred_element_type=jnp.float32
    )


def flip(tile):
    return jnp.transpose(tile.astype(jnp.float32))


def pair_body(
    tokens, heads, group, lengths_hbm, q_hbm, g_hbm, k_hbm, v_hbm, dq, dk, dv,
    qx, gx, kx, vx, kd, vd, bias, probs, outs, probs_low, score_low, flat, turned, inverses, peaks, acc, part, away, back,
    lengths_ref, lengths_sem, kv_sem, own_sem, kv_swap_send, kv_swap_recv, swap_send, swap_recv,
    doc_send, doc_recv, term_send, term_recv, part_send, part_recv, out_send, out_recv,
):
    me = lax.axis_index("sp")
    chip = me // CORES
    core = lax.rem(me, CORES)
    other = 1 - core
    sibling = chip * CORES + other
    rows = tokens * CORES
    wide = group * HD
    pairs = group // 2
    scaling = 1.0 / math.sqrt(HD)

    def cols(half, j, width):
        return pl.ds(pl.multiple_of((half * heads + j) * width, width), width)

    def remote(src, dst, send, recv, device):
        return pltpu.make_async_remote_copy(
            src_ref=src, dst_ref=dst, send_sem=send, recv_sem=recv,
            device_id={"sp": device}, device_id_type=MESH,
        )

    kv_own = [
        pltpu.make_async_copy(src, dst.at[core], kv_sem.at[i])
        for i, (src, dst) in enumerate(((k_hbm, kx), (v_hbm, vx)))
    ]

    def own_copies(j, which):
        half = (core, other)[which]
        return [
            pltpu.make_async_copy(
                src.at[:, cols(half, j, wide)], dst.at[core, :, cols(half, j, wide)],
                own_sem.at[i, which, j],
            )
            for i, (src, dst) in enumerate(((q_hbm, qx), (g_hbm, gx)))
        ]

    kv_half = pl.ds(pl.multiple_of(other * heads * HD, heads * HD), heads * HD)
    kv_swap = [
        remote(
            ref.at[core, :, kv_half], ref.at[core, :, kv_half],
            kv_swap_send.at[i], kv_swap_recv.at[i], sibling,
        )
        for i, ref in enumerate((kx, vx))
    ]

    def swap_copies(j):
        return [
            remote(
                ref.at[core, :, cols(other, j, wide)], ref.at[core, :, cols(other, j, wide)],
                swap_send.at[i, j], swap_recv.at[i, j], sibling,
            )
            for i, ref in enumerate((qx, gx))
        ]

    def doc_copies(j, i, source_core):
        from_rows = pl.ds(pl.multiple_of(source_core * tokens, tokens), tokens)
        src, dst = ((kx, kd), (vx, vd))[i]
        return [
            remote(
                src.at[source_core, :, cols(half, j, HD)], dst.at[j, from_rows],
                doc_send.at[half, i, j], doc_recv.at[source_core, i, j], CORES + half,
            )
            for half in range(CORES)
        ]

    def term_copies(j, i, half):
        return [
            remote(
                away.at[i, j, pl.ds(keeper * tokens, tokens)], back.at[i, half, j],
                term_send.at[i, keeper, j], term_recv.at[i, half, j], keeper,
            )
            for keeper in range(CORES)
        ]

    def part_copy(j, i):
        return remote(
            part.at[i, j], acc.at[i, core, j], part_send.at[i, j], part_recv.at[i, j], sibling
        )

    def out_copy(j, i):
        ref, width = ((dq, wide), (dk, HD), (dv, HD))[i]
        view = ref.at[other, :, cols(core, j, width)]
        return remote(view, view, out_send.at[i, j], out_recv.at[i, j], sibling)

    barrier = pltpu.get_barrier_semaphore()
    for step in range(1, 2 * CORES):
        pl.semaphore_signal(
            barrier, inc=1, device_id={"sp": lax.rem(me + step, 2 * CORES)}, device_id_type=MESH
        )
    lengths_copy = pltpu.make_async_copy(lengths_hbm, lengths_ref, lengths_sem)
    for copy in kv_own:
        copy.start()

    def load_rows():
        lengths_copy.start()
        for j in range(heads):
            for copy in own_copies(j, 1) + own_copies(j, 0):
                copy.start()

    sends = [copy for j in range(heads) for i in range(2) for copy in doc_copies(j, i, core)]

    @pl.when(chip == 0)
    def _():
        pl.semaphore_wait(barrier, 2 * CORES - 1)
        for copy in kv_own:
            copy.wait()
        for copy in sends[:WINDOW]:
            copy.start()
        load_rows()

    @pl.when(chip == 1)
    def _():
        load_rows()
        pl.semaphore_wait(barrier, 2 * CORES - 1)
        for copy in kv_own:
            copy.wait()

    for copy in kv_swap:
        copy.start()
    for j in range(heads):
        for copy in own_copies(j, 1):
            copy.wait()
        for copy in swap_copies(j):
            copy.start()

    @pl.when(chip == 0)
    def _():
        for copy in sends[WINDOW:]:
            copy.start()

    lengths_copy.wait()
    places = chip * rows + lax.broadcasted_iota(jnp.int32, (1, rows), 1)
    doc_len = rows
    asked = places - doc_len
    start = jnp.zeros((1, rows), jnp.int32)
    end = jnp.int32(0)
    for c in range(lengths_ref.shape[0]):
        end = end + lengths_ref[c]
        start = jnp.where(end <= asked, end, start)
    first = jnp.where(asked < 0, 0, start + doc_len)
    key_places = chip * rows + lax.broadcasted_iota(jnp.int32, (rows, rows), 0)
    query_places = chip * rows + lax.broadcasted_iota(jnp.int32, (rows, rows), 1)
    seen = (key_places <= query_places) & (key_places >= first)
    bias[...] = jnp.where(seen, 0.0, MASKED)

    for copy in kv_swap:
        copy.wait()

    tiles = [(a, p) for a in range(CORES) for p in range(pairs)]

    def head_cols(j, h):
        return pl.ds(pl.multiple_of((core * heads + j) * wide + h * HD, HD), HD)

    def block(ref, j, a, p):
        return jnp.concatenate(
            [ref[a, :, head_cols(j, 2 * p)], ref[a, :, head_cols(j, 2 * p + 1)]], axis=0
        )

    def whole(ref, j, first_a):
        return jnp.concatenate(
            [block(ref, j, a, p) for a, p in tiles if a >= first_a], axis=0
        )

    def own(ref, j, a):
        return ref[: a + 1, :, cols(core, j, HD)].reshape((a + 1) * tokens, HD)

    def span(n):
        return slice(n * rows, (n + 1) * rows)

    def arrive(j):
        for copy in own_copies(j, 0) + swap_copies(j):
            copy.wait()

    def own_scores(j, low):
        for n, (a, p) in enumerate(tiles):
            seen_keys = (a + 1) * tokens
            raw = dot(own(kx, j, a), block(qx, j, a, p), 1, 1)
            mask = bias[:seen_keys, a * tokens : (a + 1) * tokens]
            raw = raw + jnp.concatenate([mask, mask], axis=1)
            probs[n, low : low + seen_keys] = raw
            peaks[n] = fold(raw, jnp.max)
            flat[:, span(n)] = flip(block(gx, j, a, p)).astype(jnp.bfloat16)
        turned[:, low : low + rows] = flip(own(vx, j, CORES - 1)).astype(jnp.bfloat16)

    def own_outputs(j, low):
        for n, (a, p) in enumerate(tiles):
            extent = low + (a + 1) * tokens
            outs[n] = dot(turned[:, low:extent], probs_low[low:extent, span(n)], 1, 0)

    def fold(chunk, op):
        return op(chunk.reshape(chunk.shape[0] // 8, 8, chunk.shape[1]), axis=0)

    def normalize(j, low):
        if low:
            for n, (a, p) in enumerate(tiles):
                probs[n, :low] = dot(kd[j], block(qx, j, a, p), 1, 1)
        for n, (a, p) in enumerate(tiles):
            extent = low + (a + 1) * tokens
            peak = peaks[n]
            for r in range(0, low, CHUNK):
                peak = jnp.maximum(peak, fold(probs[n, r : r + CHUNK], jnp.max))
            peak = jnp.max(peak, axis=0, keepdims=True)
            total = None
            for r in range(0, extent, CHUNK):
                weight = jnp.exp2((probs[n, r : r + CHUNK] - peak) * (scaling * math.log2(math.e)))
                probs_low[r : r + CHUNK, span(n)] = weight.astype(jnp.bfloat16)
                part_total = fold(weight, jnp.sum)
                total = part_total if total is None else total + part_total
            inverse = 1.0 / jnp.sum(total, axis=0, keepdims=True)
            inverses[n] = jnp.broadcast_to(inverse, (8, rows))
            flat[:, span(n)] = (flat[:, span(n)].astype(jnp.float32) * inverse).astype(jnp.bfloat16)

    def deltas(j, low):
        if low:
            turned[:, :low] = flip(vd[j]).astype(jnp.bfloat16)
        for n, (a, p) in enumerate(tiles):
            output = outs[n]
            if low:
                output = output + dot(turned[:, :low], probs_low[:low, span(n)], 1, 0)
            delta = jnp.sum(output * flat[:, span(n)].astype(jnp.float32), axis=0, keepdims=True)
            inverses[n] = inverses[n] * delta

    def differentiate(j, start, keys_of):
        for n, (a, p) in enumerate(tiles):
            values = keys_of(a)
            here = slice(start, start + values.shape[0])
            grad = dot(values, flat[:, span(n)], 1, 0)
            single = probs_low[here, span(n)].astype(jnp.float32)
            score_low[here, span(n)] = (single * (grad - inverses[n, :1])).astype(jnp.bfloat16)

    def doc_sum(low_ref, other, j):
        if low_ref is probs_low:
            return dot(low_ref[:rows], flat[...], 1, 1)
        return dot(low_ref[:rows], whole(other, j, 0), 1, 0)

    def sum_over(low_ref, other, j, low):
        sums = []
        for b in range(CORES):
            left = low_ref[low + b * tokens : low + (b + 1) * tokens, b * pairs * rows :]
            if low_ref is probs_low:
                sums.append(dot(left, flat[:, b * pairs * rows :], 1, 1))
            else:
                sums.append(dot(left, whole(other, j, b), 1, 0))
        return sums

    def query_grads(j, low):
        keys = own(kx, j, CORES - 1)
        if low:
            keys = jnp.concatenate([kd[j], keys], axis=0)
        keys_flat = flip(keys).astype(jnp.bfloat16)
        for n, (a, p) in enumerate(tiles):
            extent = low + (a + 1) * tokens
            result = dot(keys_flat[:, :extent], score_low[:extent, span(n)], 1, 0) * scaling
            for h in range(2):
                dq[a, :, head_cols(j, 2 * p + h)] = jnp.transpose(
                    result[:, h * tokens : (h + 1) * tokens]
                ).astype(jnp.bfloat16)

    @pl.when(chip == 0)
    def _():
        def keep(i, j, low, high):
            acc[i, core, j] = jnp.where(core == 0, low, high)
            part[i, j] = jnp.where(core == 0, high, low)
            part_copy(j, i).start()

        def step(j, carry):
            arrive(j)
            own_scores(j, 0)
            normalize(j, 0)
            own_outputs(j, 0)
            low, high = sum_over(probs_low, gx, j, 0)
            keep(1, j, low, high)
            deltas(j, 0)
            differentiate(j, 0, lambda a: own(vx, j, a))
            low, high = sum_over(score_low, qx, j, 0)
            keep(0, j, low * scaling, high * scaling)
            query_grads(j, 0)
            out_copy(j, 0).start()
            return carry

        lax.fori_loop(0, heads, step, 0)

        def finish(j, carry):
            for i in (1, 0):
                part_copy(j, i).wait()
                for half in range(CORES):
                    term_copies(j, i, half)[0].wait_recv()
                    total = acc[i, half, j] + back[i, half, j].astype(jnp.float32)
                    (dk, dv)[i][core, :, cols(half, j, HD)] = total.astype(jnp.bfloat16)
            return carry

        lax.fori_loop(0, heads, finish, 0)
        for j in range(heads):
            out_copy(j, 0).wait()
        for copy in sends:
            copy.wait_send()

    @pl.when(chip == 1)
    def _():
        def step(j, carry):
            arrive(j)
            own_scores(j, rows)
            for source_core in range(CORES):
                doc_copies(j, 0, source_core)[0].wait_recv()
            normalize(j, rows)
            away[1, j] = doc_sum(probs_low, gx, j).astype(jnp.bfloat16)
            for copy in term_copies(j, 1, core):
                copy.start()
            own_outputs(j, rows)
            for a, total in enumerate(sum_over(probs_low, gx, j, rows)):
                dv[a, :, cols(core, j, HD)] = total.astype(jnp.bfloat16)
            for source_core in range(CORES):
                doc_copies(j, 1, source_core)[0].wait_recv()
            deltas(j, rows)
            differentiate(j, 0, lambda a: vd[j])
            away[0, j] = (doc_sum(score_low, qx, j) * scaling).astype(
                jnp.bfloat16
            )
            for copy in term_copies(j, 0, core):
                copy.start()
            differentiate(j, rows, lambda a: own(vx, j, a))
            for a, total in enumerate(sum_over(score_low, qx, j, rows)):
                dk[a, :, cols(core, j, HD)] = (total * scaling).astype(jnp.bfloat16)
            query_grads(j, rows)
            for i in range(3):
                out_copy(j, i).start()
            return carry

        lax.fori_loop(0, heads, step, 0)
        for j in range(heads):
            for i in range(2):
                for copy in term_copies(j, i, core):
                    copy.wait_send()
            for i in range(3):
                out_copy(j, i).wait()


def pair_kernel(tokens, heads, group, *refs):
    sems = lambda *shape: pltpu.SemaphoreType.DMA(shape)
    pl.run_scoped(
        lambda *scoped: pair_body(tokens, heads, group, *refs, *scoped),
        pltpu.SemaphoreType.DMA,
        sems(2),
        sems(2, CORES, heads),
        sems(2),
        sems(2),
        sems(2, heads),
        sems(2, heads),
        sems(CORES, 2, heads),
        sems(CORES, 2, heads),
        sems(2, CORES, heads),
        sems(2, CORES, heads),
        sems(2, heads),
        sems(2, heads),
        sems(3, heads),
        sems(3, heads),
    )


def publish_kernel(*refs):
    pl.run_scoped(partial(publish_body, *refs), pltpu.SemaphoreType.DMA((3,)))


def publish_body(dq_in, dk_in, dv_in, dq_out, dk_out, dv_out, sem):
    core = lax.rem(lax.axis_index("sp"), CORES)
    copies = [
        pltpu.make_async_copy(src.at[core], dst, sem.at[i])
        for i, (src, dst) in enumerate(((dq_in, dq_out), (dk_in, dk_out), (dv_in, dv_out)))
    ]
    for copy in copies:
        copy.start()
    for copy in copies:
        copy.wait()


def on_pairs(query_rows, key_rows, value_rows, out_grad, question_lengths):
    tokens = query_rows.shape[0]
    heads = KVH // CORES
    group = QH // KVH
    rows = tokens * CORES
    low, wide = jnp.bfloat16, jnp.float32
    vmem, sems = pltpu.VMEM, lambda *shape: pltpu.SemaphoreType.DMA(shape)
    anywhere = pl.BlockSpec(memory_space=pl.ANY)
    tiles = group * CORES // 2
    grads = pl.pallas_call(
        partial(pair_kernel, tokens, heads, group),
        out_shape=tuple(
            pltpu.VMEM((CORES,) + array.shape, low) for array in (query_rows, key_rows, value_rows)
        ),
        in_specs=[anywhere] * 5,
        out_specs=(pl.BlockSpec(memory_space=pltpu.VMEM),) * 3,
        scratch_shapes=[
            vmem((CORES,) + query_rows.shape, low),
            vmem((CORES,) + query_rows.shape, low),
            vmem((CORES,) + key_rows.shape, low),
            vmem((CORES,) + key_rows.shape, low),
            vmem((heads, rows, HD), low),
            vmem((heads, rows, HD), low),
            vmem((rows, rows), wide),
            vmem((tiles, 2 * rows, rows), wide),
            vmem((tiles, HD, rows), wide),
            vmem((2 * rows, tiles * rows), low),
            vmem((2 * rows, tiles * rows), low),
            vmem((HD, tiles * rows), low),
            vmem((HD, 2 * rows), low),
            vmem((tiles, 8, rows), wide),
            vmem((tiles, 8, rows), wide),
            vmem((2, CORES, heads, tokens, HD), wide),
            vmem((2, heads, tokens, HD), wide),
            vmem((2, heads, rows, HD), low),
            vmem((2, CORES, heads, tokens, HD), low),
            pltpu.SMEM(question_lengths.shape, jnp.int32),
        ],
        compiler_params=pltpu.CompilerParams(
            collective_id=0, has_side_effects=True,
        ),
    )(question_lengths, query_rows, out_grad, key_rows, value_rows)
    return pl.pallas_call(
        publish_kernel,
        out_shape=tuple(
            jax.ShapeDtypeStruct(array.shape, low) for array in (query_rows, key_rows, value_rows)
        ),
        in_specs=[anywhere] * 3,
        out_specs=(anywhere,) * 3,
        compiler_params=pltpu.CompilerParams(has_side_effects=True, vmem_limit_bytes=1024 * 1024),
    )(*grads)


def solution(mesh):
    body = on_pairs if mesh.shape["sp"] == 2 * CORES else on_device
    return jax.shard_map(
        body,
        mesh=mesh,
        in_specs=(
            P(("grp", "sp"), None),
            P(("grp", "sp"), None),
            P(("grp", "sp"), None),
            P(("grp", "sp"), None),
            P("grp"),
        ),
        out_specs=(P(("grp", "sp"), None), P(("grp", "sp"), None), P(("grp", "sp"), None)),
        check_vma=False,
    )
```

```python
from functools import partial
from functools import reduce
import math

import jax
import jax.numpy as jnp
from jax import lax
from jax.experimental import pallas as pl
from jax.experimental.pallas import tpu as pltpu
from jax.sharding import PartitionSpec as P

HD = 128
QH = 32
KVH = 8


MASKED = -1e30


def widen(rows, copies):
    tokens = rows.shape[0]
    shaped = rows.reshape(tokens, KVH, 1, HD)
    return jnp.broadcast_to(shaped, (tokens, KVH, copies, HD)).reshape(tokens, KVH * copies * HD)


def segment_ids(question_lengths, length, doc_len):
    ends = jnp.cumsum(question_lengths)
    places = jnp.arange(length, dtype=jnp.int32)
    inside = jnp.sum((ends[None, :] <= (places - doc_len)[:, None]).astype(jnp.int32), axis=1)
    return jnp.where(places < doc_len, -1, inside)


def make_scores(query_block, key_block, visible, scaling):
    raw = (
        jnp.einsum("bkgd,skd->kgbs", query_block, key_block, preferred_element_type=jnp.float32)
        * scaling
    )
    return jnp.where(visible[None, None], raw, MASKED)


def weighted_values(probs_b, value_block):
    return jnp.einsum("kgbs,skd->bkgd", probs_b, value_block, preferred_element_type=jnp.float32)


def backward_block(probs, probs_b, delta, grad_block, query_block, key_block, value_block, scaling):
    value_part = jnp.einsum(
        "kgbs,bkgd->skd", probs_b, grad_block, preferred_element_type=jnp.float32
    )
    prob_grad = jnp.einsum(
        "bkgd,skd->kgbs", grad_block, value_block, preferred_element_type=jnp.float32
    )
    score_grad = (probs * (prob_grad - delta[..., None])).astype(jnp.bfloat16)
    query_part = jnp.einsum(
        "kgbs,skd->bkgd", score_grad, key_block, preferred_element_type=jnp.float32
    )
    key_part = (
        jnp.einsum("kgbs,bkgd->skd", score_grad, query_block, preferred_element_type=jnp.float32)
        * scaling
    )
    return (query_part, key_part, value_part)


def on_device(query_rows, key_rows, value_rows, out_grad, question_lengths):
    devices = lax.axis_size("sp")
    tokens = query_rows.shape[0]
    length = tokens * devices
    doc_len = length // 2
    block_len = min(512, length)
    block_count = length // block_len
    scaling = 1.0 / math.sqrt(HD)
    copies = max(KVH, devices) // KVH
    keys_local, values_local = (
        lax.all_to_all(widen(key_rows, copies), "sp", split_axis=1, concat_axis=0, tiled=True),
        lax.all_to_all(widen(value_rows, copies), "sp", split_axis=1, concat_axis=0, tiled=True),
    )
    queries_local, grads_local = (
        lax.all_to_all(query_rows, "sp", split_axis=1, concat_axis=0, tiled=True),
        lax.all_to_all(out_grad, "sp", split_axis=1, concat_axis=0, tiled=True),
    )
    key_heads = KVH * copies // devices
    per_group = QH // devices // key_heads
    queries = queries_local.reshape(length, key_heads, per_group, HD)
    grads = grads_local.reshape(length, key_heads, per_group, HD)
    keys = keys_local.reshape(length, key_heads, HD)
    values = values_local.reshape(length, key_heads, HD)
    segment = segment_ids(question_lengths, length, doc_len)
    places = jnp.arange(length, dtype=jnp.int32)
    query_shape = (block_len, key_heads, per_group, HD)
    key_shape = (block_len, key_heads, HD)
    key_sums = [jnp.zeros(key_shape, jnp.float32)] * block_count
    value_sums = [jnp.zeros(key_shape, jnp.float32)] * block_count
    query_parts = []
    for row_block in range(block_count):
        row_start = row_block * block_len
        query_block = queries[row_start : row_start + block_len]
        grad_block = grads[row_start : row_start + block_len]
        row_places = places[row_start : row_start + block_len]
        row_segment = segment[row_start : row_start + block_len]
        needs = []
        scores = []
        for col_block in range(row_block + 1):
            col_start = col_block * block_len
            col_places = places[col_start : col_start + block_len]
            col_segment = segment[col_start : col_start + block_len]
            visible = (col_places[None, :] <= row_places[:, None]) & (
                (col_places[None, :] < doc_len) | (col_segment[None, :] == row_segment[:, None])
            )
            needed = True
            needs.append(needed)
            scores.append(
                make_scores(query_block, keys[col_start : col_start + block_len], visible, scaling)
            )
        peak = reduce(jnp.maximum, [jnp.max(score, axis=3) for score in scores])
        total = reduce(
            jnp.add, [jnp.sum(jnp.exp(score - peak[..., None]), axis=3) for score in scores]
        )
        log_total = peak + jnp.log(total)
        probs = [jnp.exp(score - log_total[..., None]) for score in scores]
        probs_low = [single.astype(jnp.bfloat16) for single in probs]
        output = jnp.zeros(query_shape, jnp.float32)
        for col_block in range(row_block + 1):
            col_start = col_block * block_len
            output = output + weighted_values(
                probs_low[col_block], values[col_start : col_start + block_len]
            )
        output_low = output.astype(jnp.bfloat16)
        delta = jnp.einsum(
            "bkgd,bkgd->kgb", grad_block, output_low, preferred_element_type=jnp.float32
        )
        query_sum = jnp.zeros(query_shape, jnp.float32)
        for col_block in range(row_block + 1):
            col_start = col_block * block_len
            action = partial(
                backward_block,
                probs[col_block],
                probs_low[col_block],
                delta,
                grad_block,
                query_block,
                keys[col_start : col_start + block_len],
                values[col_start : col_start + block_len],
                scaling,
            )
            query_part, key_part, value_part = action()
            query_sum = query_sum + query_part
            key_sums[col_block] = key_sums[col_block] + key_part
            value_sums[col_block] = value_sums[col_block] + value_part
        query_parts.append((query_sum * scaling).astype(jnp.bfloat16))
    query_local = jnp.concatenate(query_parts, axis=0).reshape(length, key_heads * per_group * HD)
    key_local = jnp.concatenate(key_sums, axis=0).reshape(length, key_heads * HD)
    value_local = jnp.concatenate(value_sums, axis=0).reshape(length, key_heads * HD)
    query_grad = lax.all_to_all(query_local, "sp", split_axis=0, concat_axis=1, tiled=True)
    key_back, value_back = (
        lax.all_to_all(key_local, "sp", split_axis=0, concat_axis=1, tiled=True),
        lax.all_to_all(value_local, "sp", split_axis=0, concat_axis=1, tiled=True),
    )
    key_grad = (
        jnp.sum(key_back.reshape(tokens, KVH, copies, HD), axis=2)
        .reshape(tokens, KVH * HD)
        .astype(jnp.bfloat16)
    )
    value_grad = (
        jnp.sum(value_back.reshape(tokens, KVH, copies, HD), axis=2)
        .reshape(tokens, KVH * HD)
        .astype(jnp.bfloat16)
    )
    return (query_grad, key_grad, value_grad)


MESH = pl.DeviceIdType.MESH
CORES = 2
CHUNK = 64
WINDOW = 4


def dot(left, right, left_dim, right_dim):
    return lax.dot_general(
        left, right, (((left_dim,), (right_dim,)), ((), ())), preferred_element_type=jnp.float32
    )


def flip(tile):
    return jnp.transpose(tile.astype(jnp.float32))


def pair_body(
    tokens, heads, group, lengths_hbm, q_hbm, g_hbm, k_hbm, v_hbm, dq, dk, dv,
    qx, gx, kx, vx, kd, vd, bias, probs, outs, probs_low, score_low, flat, queries, turned, inverses, peaks, acc, part, away, back,
    lengths_ref, lengths_sem, kv_sem, own_sem, kv_swap_send, kv_swap_recv, swap_send, swap_recv,
    doc_send, doc_recv, term_send, term_recv, part_send, part_recv, out_send, out_recv,
):
    me = lax.axis_index("sp")
    chip = me // CORES
    core = lax.rem(me, CORES)
    other = 1 - core
    sibling = chip * CORES + other
    rows = tokens * CORES
    wide = group * HD
    pairs = group // 2
    scaling = 1.0 / math.sqrt(HD)

    def cols(half, j, width):
        return pl.ds(pl.multiple_of((half * heads + j) * width, width), width)

    def remote(src, dst, send, recv, device):
        return pltpu.make_async_remote_copy(
            src_ref=src, dst_ref=dst, send_sem=send, recv_sem=recv,
            device_id={"sp": device}, device_id_type=MESH,
        )

    kv_own = [
        pltpu.make_async_copy(src, dst.at[core], kv_sem.at[i])
        for i, (src, dst) in enumerate(((k_hbm, kx), (v_hbm, vx)))
    ]

    def own_copies(j, which):
        half = (core, other)[which]
        return [
            pltpu.make_async_copy(
                src.at[:, cols(half, j, wide)], dst.at[core, :, cols(half, j, wide)],
                own_sem.at[i, which, j],
            )
            for i, (src, dst) in enumerate(((q_hbm, qx), (g_hbm, gx)))
        ]

    kv_half = pl.ds(pl.multiple_of(other * heads * HD, heads * HD), heads * HD)
    kv_swap = [
        remote(
            ref.at[core, :, kv_half], ref.at[core, :, kv_half],
            kv_swap_send.at[i], kv_swap_recv.at[i], sibling,
        )
        for i, ref in enumerate((kx, vx))
    ]

    def swap_copies(j):
        return [
            remote(
                ref.at[core, :, cols(other, j, wide)], ref.at[core, :, cols(other, j, wide)],
                swap_send.at[i, j], swap_recv.at[i, j], sibling,
            )
            for i, ref in enumerate((qx, gx))
        ]

    def doc_copies(j, i, source_core):
        from_rows = pl.ds(pl.multiple_of(source_core * tokens, tokens), tokens)
        src, dst = ((kx, kd), (vx, vd))[i]
        return [
            remote(
                src.at[source_core, :, cols(half, j, HD)], dst.at[j, from_rows],
                doc_send.at[half, i, j], doc_recv.at[source_core, i, j], CORES + half,
            )
            for half in range(CORES)
        ]

    def term_copies(j, i, half):
        return [
            remote(
                away.at[i, j, pl.ds(keeper * tokens, tokens)], back.at[i, half, j],
                term_send.at[i, keeper, j], term_recv.at[i, half, j], keeper,
            )
            for keeper in range(CORES)
        ]

    def part_copy(j, i):
        return remote(
            part.at[i, j], acc.at[i, core, j], part_send.at[i, j], part_recv.at[i, j], sibling
        )

    def out_copy(j, i):
        ref, width = ((dq, wide), (dk, HD), (dv, HD))[i]
        view = ref.at[other, :, cols(core, j, width)]
        return remote(view, view, out_send.at[i, j], out_recv.at[i, j], sibling)

    barrier = pltpu.get_barrier_semaphore()
    for step in range(1, 2 * CORES):
        pl.semaphore_signal(
            barrier, inc=1, device_id={"sp": lax.rem(me + step, 2 * CORES)}, device_id_type=MESH
        )
    lengths_copy = pltpu.make_async_copy(lengths_hbm, lengths_ref, lengths_sem)
    for copy in kv_own:
        copy.start()

    def load_rows():
        lengths_copy.start()
        for j in range(heads):
            for copy in own_copies(j, 1) + own_copies(j, 0):
                copy.start()

    sends = [copy for j in range(heads) for i in range(2) for copy in doc_copies(j, i, core)]

    @pl.when(chip == 0)
    def _():
        pl.semaphore_wait(barrier, 2 * CORES - 1)
        for copy in kv_own:
            copy.wait()
        for copy in sends[:WINDOW]:
            copy.start()
        load_rows()

    @pl.when(chip == 1)
    def _():
        load_rows()
        pl.semaphore_wait(barrier, 2 * CORES - 1)
        for copy in kv_own:
            copy.wait()

    for copy in kv_swap:
        copy.start()
    for j in range(heads):
        for copy in own_copies(j, 1):
            copy.wait()
        for copy in swap_copies(j):
            copy.start()

    @pl.when(chip == 0)
    def _():
        for copy in sends[WINDOW:]:
            copy.start()

    lengths_copy.wait()
    places = chip * rows + lax.broadcasted_iota(jnp.int32, (1, rows), 1)
    doc_len = rows
    asked = places - doc_len
    start = jnp.zeros((1, rows), jnp.int32)
    end = jnp.int32(0)
    for c in range(lengths_ref.shape[0]):
        end = end + lengths_ref[c]
        start = jnp.where(end <= asked, end, start)
    first = jnp.where(asked < 0, 0, start + doc_len)
    key_places = chip * rows + lax.broadcasted_iota(jnp.int32, (rows, rows), 0)
    query_places = chip * rows + lax.broadcasted_iota(jnp.int32, (rows, rows), 1)
    seen = (key_places <= query_places) & (key_places >= first)
    bias[...] = jnp.where(seen, 0.0, MASKED)

    for copy in kv_swap:
        copy.wait()

    tiles = [(a, p) for a in range(CORES) for p in range(pairs)]

    def head_cols(j, h):
        return pl.ds(pl.multiple_of((core * heads + j) * wide + h * HD, HD), HD)

    def block(ref, j, a, p):
        return jnp.concatenate(
            [ref[a, :, head_cols(j, 2 * p)], ref[a, :, head_cols(j, 2 * p + 1)]], axis=0
        )

    def own(ref, j, a):
        return ref[: a + 1, :, cols(core, j, HD)].reshape((a + 1) * tokens, HD)

    def put(ref, here, n, value):
        for h in range(2):
            ref[2 * n + h, here] = value[:, h * HD : (h + 1) * HD]

    def get(ref, here, n):
        return jnp.concatenate([ref[2 * n, here], ref[2 * n + 1, here]], axis=1)

    def tail(ref, here, b):
        return jnp.concatenate(
            [ref[h, here] for h in range(2 * b * pairs, 2 * len(tiles))], axis=1
        )

    def arrive(j):
        for copy in own_copies(j, 0) + swap_copies(j):
            copy.wait()

    def own_scores(j, low):
        for n, (a, p) in enumerate(tiles):
            queries[n] = block(qx, j, a, p)
            seen_keys = (a + 1) * tokens
            raw = dot(own(kx, j, a), queries[n], 1, 1)
            mask = bias[:seen_keys, a * tokens : (a + 1) * tokens]
            raw = raw + jnp.concatenate([mask, mask], axis=1)
            probs[n, low : low + seen_keys] = raw
            peaks[n] = fold(raw, jnp.max)
            put(flat, slice(None), n, flip(block(gx, j, a, p)).astype(jnp.bfloat16))
        turned[:, low : low + rows] = flip(own(vx, j, CORES - 1)).astype(jnp.bfloat16)

    def own_outputs(j, low):
        for n, (a, p) in enumerate(tiles):
            extent = low + (a + 1) * tokens
            outs[n] = dot(turned[:, low:extent], get(probs_low, slice(low, extent), n), 1, 0)

    def fold(chunk, op):
        return op(chunk.reshape(chunk.shape[0] // 8, 8, chunk.shape[1]), axis=0)

    def normalize(j, low):
        if low:
            for n, (a, p) in enumerate(tiles):
                probs[n, :low] = dot(kd[j], queries[n], 1, 1)
        for n, (a, p) in enumerate(tiles):
            extent = low + (a + 1) * tokens
            peak = peaks[n]
            for r in range(0, low, CHUNK):
                peak = jnp.maximum(peak, fold(probs[n, r : r + CHUNK], jnp.max))
            peak = jnp.max(peak, axis=0, keepdims=True)
            total = None
            for r in range(0, extent, CHUNK):
                weight = jnp.exp2((probs[n, r : r + CHUNK] - peak) * (scaling * math.log2(math.e)))
                put(probs_low, slice(r, r + CHUNK), n, weight.astype(jnp.bfloat16))
                part_total = fold(weight, jnp.sum)
                total = part_total if total is None else total + part_total
            inverse = 1.0 / jnp.sum(total, axis=0, keepdims=True)
            inverses[n] = jnp.broadcast_to(inverse, (8, rows))
            scaled = get(flat, slice(None), n).astype(jnp.float32) * inverse
            put(flat, slice(None), n, scaled.astype(jnp.bfloat16))

    def deltas(j, low):
        if low:
            turned[:, :low] = flip(vd[j]).astype(jnp.bfloat16)
        for n, (a, p) in enumerate(tiles):
            output = outs[n]
            if low:
                output = output + dot(turned[:, :low], get(probs_low, slice(0, low), n), 1, 0)
            delta = jnp.sum(output * get(flat, slice(None), n).astype(jnp.float32), axis=0, keepdims=True)
            inverses[n] = inverses[n] * delta

    def differentiate(j, start, keys_of):
        for n, (a, p) in enumerate(tiles):
            values = keys_of(a)
            here = slice(start, start + values.shape[0])
            grad = dot(values, get(flat, slice(None), n), 1, 0)
            single = get(probs_low, here, n).astype(jnp.float32)
            score = single * (grad - inverses[n, :1])
            put(score_low, here, n, score.astype(jnp.bfloat16))

    def doc_sum(low_ref, other, j):
        if low_ref is probs_low:
            return dot(tail(low_ref, slice(0, rows), 0), tail(flat, slice(None), 0), 1, 1)
        return dot(tail(low_ref, slice(0, rows), 0), queries[...].reshape(-1, HD), 1, 0)

    def sum_over(low_ref, other, j, low):
        sums = []
        for b in range(CORES):
            left = tail(low_ref, slice(low + b * tokens, low + (b + 1) * tokens), b)
            if low_ref is probs_low:
                sums.append(dot(left, tail(flat, slice(None), b), 1, 1))
            else:
                sums.append(dot(left, queries[b * pairs :].reshape(-1, HD), 1, 0))
        return sums

    def query_grads(j, low):
        keys = own(kx, j, CORES - 1)
        if low:
            keys = jnp.concatenate([kd[j], keys], axis=0)
        keys_flat = flip(keys).astype(jnp.bfloat16)
        for n, (a, p) in enumerate(tiles):
            extent = low + (a + 1) * tokens
            result = dot(keys_flat[:, :extent], get(score_low, slice(0, extent), n), 1, 0) * scaling
            for h in range(2):
                dq[a, :, head_cols(j, 2 * p + h)] = jnp.transpose(
                    result[:, h * tokens : (h + 1) * tokens]
                ).astype(jnp.bfloat16)

    @pl.when(chip == 0)
    def _():
        def keep(i, j, low, high):
            acc[i, core, j] = jnp.where(core == 0, low, high)
            part[i, j] = jnp.where(core == 0, high, low)
            part_copy(j, i).start()

        def step(j, carry):
            arrive(j)
            own_scores(j, 0)
            normalize(j, 0)
            own_outputs(j, 0)
            low, high = sum_over(probs_low, gx, j, 0)
            keep(1, j, low, high)
            deltas(j, 0)
            differentiate(j, 0, lambda a: own(vx, j, a))
            low, high = sum_over(score_low, qx, j, 0)
            keep(0, j, low * scaling, high * scaling)
            query_grads(j, 0)
            out_copy(j, 0).start()
            return carry

        lax.fori_loop(0, heads, step, 0)

        def finish(j, carry):
            for i in (1, 0):
                part_copy(j, i).wait()
                for half in range(CORES):
                    term_copies(j, i, half)[0].wait_recv()
                    total = acc[i, half, j] + back[i, half, j].astype(jnp.float32)
                    (dk, dv)[i][core, :, cols(half, j, HD)] = total.astype(jnp.bfloat16)
            return carry

        for j in range(heads):
            out_copy(j, 0).wait()
        for copy in sends:
            copy.wait_send()
        lax.fori_loop(0, heads, finish, 0)

    @pl.when(chip == 1)
    def _():
        def step(j, carry):
            arrive(j)
            own_scores(j, rows)
            for source_core in range(CORES):
                doc_copies(j, 0, source_core)[0].wait_recv()
            normalize(j, rows)
            away[1, j] = doc_sum(probs_low, gx, j).astype(jnp.bfloat16)
            for copy in term_copies(j, 1, core):
                copy.start()
            own_outputs(j, rows)
            for a, total in enumerate(sum_over(probs_low, gx, j, rows)):
                dv[a, :, cols(core, j, HD)] = total.astype(jnp.bfloat16)
            for source_core in range(CORES):
                doc_copies(j, 1, source_core)[0].wait_recv()
            deltas(j, rows)
            differentiate(j, 0, lambda a: vd[j])
            away[0, j] = (doc_sum(score_low, qx, j) * scaling).astype(
                jnp.bfloat16
            )
            for copy in term_copies(j, 0, core):
                copy.start()
            differentiate(j, rows, lambda a: own(vx, j, a))
            for a, total in enumerate(sum_over(score_low, qx, j, rows)):
                dk[a, :, cols(core, j, HD)] = (total * scaling).astype(jnp.bfloat16)
            query_grads(j, rows)
            for i in range(3):
                out_copy(j, i).start()
            return carry

        lax.fori_loop(0, heads, step, 0)
        for j in range(heads):
            for i in range(2):
                for copy in term_copies(j, i, core):
                    copy.wait_send()
            for i in range(3):
                out_copy(j, i).wait()


def pair_kernel(tokens, heads, group, *refs):
    sems = lambda *shape: pltpu.SemaphoreType.DMA(shape)
    pl.run_scoped(
        lambda *scoped: pair_body(tokens, heads, group, *refs, *scoped),
        pltpu.SemaphoreType.DMA,
        sems(2),
        sems(2, CORES, heads),
        sems(2),
        sems(2),
        sems(2, heads),
        sems(2, heads),
        sems(CORES, 2, heads),
        sems(CORES, 2, heads),
        sems(2, CORES, heads),
        sems(2, CORES, heads),
        sems(2, heads),
        sems(2, heads),
        sems(3, heads),
        sems(3, heads),
    )


def publish_kernel(*refs):
    pl.run_scoped(partial(publish_body, *refs), pltpu.SemaphoreType.DMA((3,)))


def publish_body(dq_in, dk_in, dv_in, dq_out, dk_out, dv_out, sem):
    core = lax.rem(lax.axis_index("sp"), CORES)
    copies = [
        pltpu.make_async_copy(src.at[core], dst, sem.at[i])
        for i, (src, dst) in enumerate(((dq_in, dq_out), (dk_in, dk_out), (dv_in, dv_out)))
    ]
    for copy in copies:
        copy.start()
    for copy in copies:
        copy.wait()


def on_pairs(query_rows, key_rows, value_rows, out_grad, question_lengths):
    tokens = query_rows.shape[0]
    heads = KVH // CORES
    group = QH // KVH
    rows = tokens * CORES
    low, wide = jnp.bfloat16, jnp.float32
    vmem, sems = pltpu.VMEM, lambda *shape: pltpu.SemaphoreType.DMA(shape)
    anywhere = pl.BlockSpec(memory_space=pl.ANY)
    tiles = group * CORES // 2
    grads = pl.pallas_call(
        partial(pair_kernel, tokens, heads, group),
        out_shape=tuple(
            pltpu.VMEM((CORES,) + array.shape, low) for array in (query_rows, key_rows, value_rows)
        ),
        in_specs=[anywhere] * 5,
        out_specs=(pl.BlockSpec(memory_space=pltpu.VMEM),) * 3,
        scratch_shapes=[
            vmem((CORES,) + query_rows.shape, low),
            vmem((CORES,) + query_rows.shape, low),
            vmem((CORES,) + key_rows.shape, low),
            vmem((CORES,) + key_rows.shape, low),
            vmem((heads, rows, HD), low),
            vmem((heads, rows, HD), low),
            vmem((rows, rows), wide),
            vmem((tiles, 2 * rows, rows), wide),
            vmem((tiles, HD, rows), wide),
            vmem((2 * tiles, 2 * rows, HD), low),
            vmem((2 * tiles, 2 * rows, HD), low),
            vmem((2 * tiles, HD, HD), low),
            vmem((tiles, rows, HD), low),
            vmem((HD, 2 * rows), low),
            vmem((tiles, 8, rows), wide),
            vmem((tiles, 8, rows), wide),
            vmem((2, CORES, heads, tokens, HD), wide),
            vmem((2, heads, tokens, HD), wide),
            vmem((2, heads, rows, HD), low),
            vmem((2, CORES, heads, tokens, HD), low),
            pltpu.SMEM(question_lengths.shape, jnp.int32),
        ],
        compiler_params=pltpu.CompilerParams(
            collective_id=0, has_side_effects=True,
        ),
    )(question_lengths, query_rows, out_grad, key_rows, value_rows)
    return pl.pallas_call(
        publish_kernel,
        out_shape=tuple(
            jax.ShapeDtypeStruct(array.shape, low) for array in (query_rows, key_rows, value_rows)
        ),
        in_specs=[anywhere] * 3,
        out_specs=(anywhere,) * 3,
        compiler_params=pltpu.CompilerParams(has_side_effects=True, vmem_limit_bytes=1024 * 1024),
    )(*grads)


def solution(mesh):
    body = on_pairs if mesh.shape["sp"] == 2 * CORES else on_device
    return jax.shard_map(
        body,
        mesh=mesh,
        in_specs=(
            P(("grp", "sp"), None),
            P(("grp", "sp"), None),
            P(("grp", "sp"), None),
            P(("grp", "sp"), None),
            P("grp"),
        ),
        out_specs=(P(("grp", "sp"), None), P(("grp", "sp"), None), P(("grp", "sp"), None)),
        check_vma=False,
    )
```

```python
from functools import partial
from functools import reduce
import math

import jax
import jax.numpy as jnp
from jax import lax
from jax.experimental import pallas as pl
from jax.experimental.pallas import tpu as pltpu
from jax.sharding import PartitionSpec as P

HD = 128
QH = 32
KVH = 8


MASKED = -1e30


def widen(rows, copies):
    tokens = rows.shape[0]
    shaped = rows.reshape(tokens, KVH, 1, HD)
    return jnp.broadcast_to(shaped, (tokens, KVH, copies, HD)).reshape(tokens, KVH * copies * HD)


def segment_ids(question_lengths, length, doc_len):
    ends = jnp.cumsum(question_lengths)
    places = jnp.arange(length, dtype=jnp.int32)
    inside = jnp.sum((ends[None, :] <= (places - doc_len)[:, None]).astype(jnp.int32), axis=1)
    return jnp.where(places < doc_len, -1, inside)


def make_scores(query_block, key_block, visible, scaling):
    raw = (
        jnp.einsum("bkgd,skd->kgbs", query_block, key_block, preferred_element_type=jnp.float32)
        * scaling
    )
    return jnp.where(visible[None, None], raw, MASKED)


def weighted_values(probs_b, value_block):
    return jnp.einsum("kgbs,skd->bkgd", probs_b, value_block, preferred_element_type=jnp.float32)


def backward_block(probs, probs_b, delta, grad_block, query_block, key_block, value_block, scaling):
    value_part = jnp.einsum(
        "kgbs,bkgd->skd", probs_b, grad_block, preferred_element_type=jnp.float32
    )
    prob_grad = jnp.einsum(
        "bkgd,skd->kgbs", grad_block, value_block, preferred_element_type=jnp.float32
    )
    score_grad = (probs * (prob_grad - delta[..., None])).astype(jnp.bfloat16)
    query_part = jnp.einsum(
        "kgbs,skd->bkgd", score_grad, key_block, preferred_element_type=jnp.float32
    )
    key_part = (
        jnp.einsum("kgbs,bkgd->skd", score_grad, query_block, preferred_element_type=jnp.float32)
        * scaling
    )
    return (query_part, key_part, value_part)


def on_device(query_rows, key_rows, value_rows, out_grad, question_lengths):
    devices = lax.axis_size("sp")
    tokens = query_rows.shape[0]
    length = tokens * devices
    doc_len = length // 2
    block_len = min(512, length)
    block_count = length // block_len
    scaling = 1.0 / math.sqrt(HD)
    copies = max(KVH, devices) // KVH
    keys_local, values_local = (
        lax.all_to_all(widen(key_rows, copies), "sp", split_axis=1, concat_axis=0, tiled=True),
        lax.all_to_all(widen(value_rows, copies), "sp", split_axis=1, concat_axis=0, tiled=True),
    )
    queries_local, grads_local = (
        lax.all_to_all(query_rows, "sp", split_axis=1, concat_axis=0, tiled=True),
        lax.all_to_all(out_grad, "sp", split_axis=1, concat_axis=0, tiled=True),
    )
    key_heads = KVH * copies // devices
    per_group = QH // devices // key_heads
    queries = queries_local.reshape(length, key_heads, per_group, HD)
    grads = grads_local.reshape(length, key_heads, per_group, HD)
    keys = keys_local.reshape(length, key_heads, HD)
    values = values_local.reshape(length, key_heads, HD)
    segment = segment_ids(question_lengths, length, doc_len)
    places = jnp.arange(length, dtype=jnp.int32)
    query_shape = (block_len, key_heads, per_group, HD)
    key_shape = (block_len, key_heads, HD)
    key_sums = [jnp.zeros(key_shape, jnp.float32)] * block_count
    value_sums = [jnp.zeros(key_shape, jnp.float32)] * block_count
    query_parts = []
    for row_block in range(block_count):
        row_start = row_block * block_len
        query_block = queries[row_start : row_start + block_len]
        grad_block = grads[row_start : row_start + block_len]
        row_places = places[row_start : row_start + block_len]
        row_segment = segment[row_start : row_start + block_len]
        needs = []
        scores = []
        for col_block in range(row_block + 1):
            col_start = col_block * block_len
            col_places = places[col_start : col_start + block_len]
            col_segment = segment[col_start : col_start + block_len]
            visible = (col_places[None, :] <= row_places[:, None]) & (
                (col_places[None, :] < doc_len) | (col_segment[None, :] == row_segment[:, None])
            )
            needed = True
            needs.append(needed)
            scores.append(
                make_scores(query_block, keys[col_start : col_start + block_len], visible, scaling)
            )
        peak = reduce(jnp.maximum, [jnp.max(score, axis=3) for score in scores])
        total = reduce(
            jnp.add, [jnp.sum(jnp.exp(score - peak[..., None]), axis=3) for score in scores]
        )
        log_total = peak + jnp.log(total)
        probs = [jnp.exp(score - log_total[..., None]) for score in scores]
        probs_low = [single.astype(jnp.bfloat16) for single in probs]
        output = jnp.zeros(query_shape, jnp.float32)
        for col_block in range(row_block + 1):
            col_start = col_block * block_len
            output = output + weighted_values(
                probs_low[col_block], values[col_start : col_start + block_len]
            )
        output_low = output.astype(jnp.bfloat16)
        delta = jnp.einsum(
            "bkgd,bkgd->kgb", grad_block, output_low, preferred_element_type=jnp.float32
        )
        query_sum = jnp.zeros(query_shape, jnp.float32)
        for col_block in range(row_block + 1):
            col_start = col_block * block_len
            action = partial(
                backward_block,
                probs[col_block],
                probs_low[col_block],
                delta,
                grad_block,
                query_block,
                keys[col_start : col_start + block_len],
                values[col_start : col_start + block_len],
                scaling,
            )
            query_part, key_part, value_part = action()
            query_sum = query_sum + query_part
            key_sums[col_block] = key_sums[col_block] + key_part
            value_sums[col_block] = value_sums[col_block] + value_part
        query_parts.append((query_sum * scaling).astype(jnp.bfloat16))
    query_local = jnp.concatenate(query_parts, axis=0).reshape(length, key_heads * per_group * HD)
    key_local = jnp.concatenate(key_sums, axis=0).reshape(length, key_heads * HD)
    value_local = jnp.concatenate(value_sums, axis=0).reshape(length, key_heads * HD)
    query_grad = lax.all_to_all(query_local, "sp", split_axis=0, concat_axis=1, tiled=True)
    key_back, value_back = (
        lax.all_to_all(key_local, "sp", split_axis=0, concat_axis=1, tiled=True),
        lax.all_to_all(value_local, "sp", split_axis=0, concat_axis=1, tiled=True),
    )
    key_grad = (
        jnp.sum(key_back.reshape(tokens, KVH, copies, HD), axis=2)
        .reshape(tokens, KVH * HD)
        .astype(jnp.bfloat16)
    )
    value_grad = (
        jnp.sum(value_back.reshape(tokens, KVH, copies, HD), axis=2)
        .reshape(tokens, KVH * HD)
        .astype(jnp.bfloat16)
    )
    return (query_grad, key_grad, value_grad)


MESH = pl.DeviceIdType.MESH
CORES = 2
CHUNK = 64
WINDOW = 4


def dot(left, right, left_dim, right_dim):
    return lax.dot_general(
        left, right, (((left_dim,), (right_dim,)), ((), ())), preferred_element_type=jnp.float32
    )


def flip(tile):
    return jnp.transpose(tile.astype(jnp.float32))


def pair_body(
    tokens, heads, group, lengths_hbm, q_hbm, g_hbm, k_hbm, v_hbm, dq, dk, dv,
    qx, gx, kx, vx, kd, vd, bias, probs, outs, probs_low, score_low, flat, queries, turned, inverses, peaks, acc, part, away, back,
    lengths_ref, lengths_sem, kv_sem, own_sem, swap_send, swap_recv,
    doc_send, doc_recv, term_send, term_recv, part_send, part_recv, out_send, out_recv,
):
    me = lax.axis_index("sp")
    chip = me // CORES
    core = lax.rem(me, CORES)
    other = 1 - core
    sibling = chip * CORES + other
    rows = tokens * CORES
    wide = group * HD
    pairs = group // 2
    scaling = 1.0 / math.sqrt(HD)

    def cols(half, j, width):
        return pl.ds(pl.multiple_of((half * heads + j) * width, width), width)

    def remote(src, dst, send, recv, device):
        return pltpu.make_async_remote_copy(
            src_ref=src, dst_ref=dst, send_sem=send, recv_sem=recv,
            device_id={"sp": device}, device_id_type=MESH,
        )

    kv_own = [
        pltpu.make_async_copy(src, dst.at[core], kv_sem.at[i])
        for i, (src, dst) in enumerate(((k_hbm, kx), (v_hbm, vx)))
    ]

    def own_copies(j, which):
        half = (core, other)[which]
        return [
            pltpu.make_async_copy(
                src.at[:, cols(half, j, wide)], dst.at[core, :, cols(half, j, wide)],
                own_sem.at[i, which, j],
            )
            for i, (src, dst) in enumerate(((q_hbm, qx), (g_hbm, gx)))
        ]

    def swap_copies(j):
        return [
            remote(
                ref.at[core, :, cols(other, j, width)], ref.at[core, :, cols(other, j, width)],
                swap_send.at[i, j], swap_recv.at[i, j], sibling,
            )
            for i, (ref, width) in enumerate(((kx, HD), (qx, wide), (gx, wide), (vx, HD)))
        ]

    def doc_copies(j, i, source_core):
        from_rows = pl.ds(pl.multiple_of(source_core * tokens, tokens), tokens)
        src, dst = ((kx, kd), (vx, vd))[i]
        return [
            remote(
                src.at[source_core, :, cols(half, j, HD)], dst.at[j, from_rows],
                doc_send.at[half, i, j], doc_recv.at[source_core, i, j], CORES + half,
            )
            for half in range(CORES)
        ]

    def term_copies(j, i, half):
        return [
            remote(
                away.at[i, j, pl.ds(keeper * tokens, tokens)], back.at[i, half, j],
                term_send.at[i, keeper, j], term_recv.at[i, half, j], keeper,
            )
            for keeper in range(CORES)
        ]

    def part_copy(j, i):
        return remote(
            part.at[i, j], acc.at[i, core, j], part_send.at[i, j], part_recv.at[i, j], sibling
        )

    def out_copy(j, i):
        ref, width = ((dq, wide), (dk, HD), (dv, HD))[i]
        view = ref.at[other, :, cols(core, j, width)]
        return remote(view, view, out_send.at[i, j], out_recv.at[i, j], sibling)

    barrier = pltpu.get_barrier_semaphore()
    for step in range(1, 2 * CORES):
        pl.semaphore_signal(
            barrier, inc=1, device_id={"sp": lax.rem(me + step, 2 * CORES)}, device_id_type=MESH
        )
    lengths_copy = pltpu.make_async_copy(lengths_hbm, lengths_ref, lengths_sem)
    for copy in kv_own:
        copy.start()

    def load_rows():
        lengths_copy.start()
        for j in range(heads):
            for copy in own_copies(j, 1) + own_copies(j, 0):
                copy.start()

    sends = [copy for j in range(heads) for i in range(2) for copy in doc_copies(j, i, core)]

    @pl.when(chip == 0)
    def _():
        pl.semaphore_wait(barrier, 2 * CORES - 1)
        for copy in kv_own:
            copy.wait()
        for copy in sends[:WINDOW]:
            copy.start()
        load_rows()

    @pl.when(chip == 1)
    def _():
        load_rows()
        pl.semaphore_wait(barrier, 2 * CORES - 1)
        for copy in kv_own:
            copy.wait()

    for j in range(heads):
        for copy in own_copies(j, 1):
            copy.wait()
        for copy in swap_copies(j):
            copy.start()

    @pl.when(chip == 0)
    def _():
        for copy in sends[WINDOW:]:
            copy.start()

    lengths_copy.wait()
    places = chip * rows + lax.broadcasted_iota(jnp.int32, (1, rows), 1)
    doc_len = rows
    asked = places - doc_len
    start = jnp.zeros((1, rows), jnp.int32)
    end = jnp.int32(0)
    for c in range(lengths_ref.shape[0]):
        end = end + lengths_ref[c]
        start = jnp.where(end <= asked, end, start)
    first = jnp.where(asked < 0, 0, start + doc_len)
    key_places = chip * rows + lax.broadcasted_iota(jnp.int32, (rows, rows), 0)
    query_places = chip * rows + lax.broadcasted_iota(jnp.int32, (rows, rows), 1)
    seen = (key_places <= query_places) & (key_places >= first)
    bias[...] = jnp.where(seen, 0.0, MASKED)

    tiles = [(a, p) for a in range(CORES) for p in range(pairs)]

    def head_cols(j, h):
        return pl.ds(pl.multiple_of((core * heads + j) * wide + h * HD, HD), HD)

    def block(ref, j, a, p):
        return jnp.concatenate(
            [ref[a, :, head_cols(j, 2 * p)], ref[a, :, head_cols(j, 2 * p + 1)]], axis=0
        )

    def own(ref, j, a):
        return ref[: a + 1, :, cols(core, j, HD)].reshape((a + 1) * tokens, HD)

    def put(ref, here, n, value):
        for h in range(2):
            ref[2 * n + h, here] = value[:, h * HD : (h + 1) * HD]

    def get(ref, here, n):
        return jnp.concatenate([ref[2 * n, here], ref[2 * n + 1, here]], axis=1)

    def tail(ref, here, b):
        return jnp.concatenate(
            [ref[h, here] for h in range(2 * b * pairs, 2 * len(tiles))], axis=1
        )

    def arrive(j):
        for copy in own_copies(j, 0) + swap_copies(j):
            copy.wait()

    def own_scores(j, low):
        for n, (a, p) in enumerate(tiles):
            queries[n] = block(qx, j, a, p)
            seen_keys = (a + 1) * tokens
            raw = dot(own(kx, j, a), queries[n], 1, 1)
            mask = bias[:seen_keys, a * tokens : (a + 1) * tokens]
            raw = raw + jnp.concatenate([mask, mask], axis=1)
            probs[n, low : low + seen_keys] = raw
            peaks[n] = fold(raw, jnp.max)
            put(flat, slice(None), n, flip(block(gx, j, a, p)).astype(jnp.bfloat16))
        turned[:, low : low + rows] = flip(own(vx, j, CORES - 1)).astype(jnp.bfloat16)

    def own_outputs(j, low):
        for n, (a, p) in enumerate(tiles):
            extent = low + (a + 1) * tokens
            outs[n] = dot(turned[:, low:extent], get(probs_low, slice(low, extent), n), 1, 0)

    def fold(chunk, op):
        return op(chunk.reshape(chunk.shape[0] // 8, 8, chunk.shape[1]), axis=0)

    def normalize(j, low):
        if low:
            for n, (a, p) in enumerate(tiles):
                probs[n, :low] = dot(kd[j], queries[n], 1, 1)
        for n, (a, p) in enumerate(tiles):
            extent = low + (a + 1) * tokens
            peak = peaks[n]
            for r in range(0, low, CHUNK):
                peak = jnp.maximum(peak, fold(probs[n, r : r + CHUNK], jnp.max))
            peak = jnp.max(peak, axis=0, keepdims=True)
            total = None
            for r in range(0, extent, CHUNK):
                weight = jnp.exp2((probs[n, r : r + CHUNK] - peak) * (scaling * math.log2(math.e)))
                put(probs_low, slice(r, r + CHUNK), n, weight.astype(jnp.bfloat16))
                part_total = fold(weight, jnp.sum)
                total = part_total if total is None else total + part_total
            inverse = 1.0 / jnp.sum(total, axis=0, keepdims=True)
            inverses[n] = jnp.broadcast_to(inverse, (8, rows))
            scaled = get(flat, slice(None), n).astype(jnp.float32) * inverse
            put(flat, slice(None), n, scaled.astype(jnp.bfloat16))

    def deltas(j, low):
        if low:
            turned[:, :low] = flip(vd[j]).astype(jnp.bfloat16)
        for n, (a, p) in enumerate(tiles):
            output = outs[n]
            if low:
                output = output + dot(turned[:, :low], get(probs_low, slice(0, low), n), 1, 0)
            delta = jnp.sum(output * get(flat, slice(None), n).astype(jnp.float32), axis=0, keepdims=True)
            inverses[n] = inverses[n] * delta

    def differentiate(j, start, keys_of):
        for n, (a, p) in enumerate(tiles):
            values = keys_of(a)
            here = slice(start, start + values.shape[0])
            grad = dot(values, get(flat, slice(None), n), 1, 0)
            single = get(probs_low, here, n).astype(jnp.float32)
            score = single * (grad - inverses[n, :1])
            put(score_low, here, n, score.astype(jnp.bfloat16))

    def doc_sum(low_ref, other, j):
        if low_ref is probs_low:
            return dot(tail(low_ref, slice(0, rows), 0), tail(flat, slice(None), 0), 1, 1)
        return dot(tail(low_ref, slice(0, rows), 0), queries[...].reshape(-1, HD), 1, 0)

    def sum_over(low_ref, other, j, low):
        sums = []
        for b in range(CORES):
            left = tail(low_ref, slice(low + b * tokens, low + (b + 1) * tokens), b)
            if low_ref is probs_low:
                sums.append(dot(left, tail(flat, slice(None), b), 1, 1))
            else:
                sums.append(dot(left, queries[b * pairs :].reshape(-1, HD), 1, 0))
        return sums

    def query_grads(j, low):
        keys = own(kx, j, CORES - 1)
        if low:
            keys = jnp.concatenate([kd[j], keys], axis=0)
        keys_flat = flip(keys).astype(jnp.bfloat16)
        for n, (a, p) in enumerate(tiles):
            extent = low + (a + 1) * tokens
            result = dot(keys_flat[:, :extent], get(score_low, slice(0, extent), n), 1, 0) * scaling
            for h in range(2):
                dq[a, :, head_cols(j, 2 * p + h)] = jnp.transpose(
                    result[:, h * tokens : (h + 1) * tokens]
                ).astype(jnp.bfloat16)

    @pl.when(chip == 0)
    def _():
        def keep(i, j, low, high):
            acc[i, core, j] = jnp.where(core == 0, low, high)
            part[i, j] = jnp.where(core == 0, high, low)
            part_copy(j, i).start()

        def step(j, carry):
            arrive(j)
            own_scores(j, 0)
            normalize(j, 0)
            own_outputs(j, 0)
            low, high = sum_over(probs_low, gx, j, 0)
            keep(1, j, low, high)
            deltas(j, 0)
            differentiate(j, 0, lambda a: own(vx, j, a))
            low, high = sum_over(score_low, qx, j, 0)
            keep(0, j, low * scaling, high * scaling)
            query_grads(j, 0)
            out_copy(j, 0).start()
            return carry

        lax.fori_loop(0, heads, step, 0)

        def finish(j, carry):
            for i in (1, 0):
                part_copy(j, i).wait()
                for half in range(CORES):
                    term_copies(j, i, half)[0].wait_recv()
                    total = acc[i, half, j] + back[i, half, j].astype(jnp.float32)
                    (dk, dv)[i][core, :, cols(half, j, HD)] = total.astype(jnp.bfloat16)
            return carry

        for j in range(heads):
            out_copy(j, 0).wait()
        for copy in sends:
            copy.wait_send()
        lax.fori_loop(0, heads, finish, 0)

    @pl.when(chip == 1)
    def _():
        def step(j, carry):
            arrive(j)
            own_scores(j, rows)
            for source_core in range(CORES):
                doc_copies(j, 0, source_core)[0].wait_recv()
            normalize(j, rows)
            away[1, j] = doc_sum(probs_low, gx, j).astype(jnp.bfloat16)
            for copy in term_copies(j, 1, core):
                copy.start()
            own_outputs(j, rows)
            for a, total in enumerate(sum_over(probs_low, gx, j, rows)):
                dv[a, :, cols(core, j, HD)] = total.astype(jnp.bfloat16)
            for source_core in range(CORES):
                doc_copies(j, 1, source_core)[0].wait_recv()
            deltas(j, rows)
            differentiate(j, 0, lambda a: vd[j])
            away[0, j] = (doc_sum(score_low, qx, j) * scaling).astype(
                jnp.bfloat16
            )
            for copy in term_copies(j, 0, core):
                copy.start()
            differentiate(j, rows, lambda a: own(vx, j, a))
            for a, total in enumerate(sum_over(score_low, qx, j, rows)):
                dk[a, :, cols(core, j, HD)] = (total * scaling).astype(jnp.bfloat16)
            query_grads(j, rows)
            for i in range(3):
                out_copy(j, i).start()
            return carry

        lax.fori_loop(0, heads, step, 0)
        for j in range(heads):
            for i in range(2):
                for copy in term_copies(j, i, core):
                    copy.wait_send()
            for i in range(3):
                out_copy(j, i).wait()


def pair_kernel(tokens, heads, group, *refs):
    sems = lambda *shape: pltpu.SemaphoreType.DMA(shape)
    pl.run_scoped(
        lambda *scoped: pair_body(tokens, heads, group, *refs, *scoped),
        pltpu.SemaphoreType.DMA,
        sems(2),
        sems(2, CORES, heads),
        sems(4, heads),
        sems(4, heads),
        sems(CORES, 2, heads),
        sems(CORES, 2, heads),
        sems(2, CORES, heads),
        sems(2, CORES, heads),
        sems(2, heads),
        sems(2, heads),
        sems(3, heads),
        sems(3, heads),
    )


def publish_kernel(*refs):
    pl.run_scoped(partial(publish_body, *refs), pltpu.SemaphoreType.DMA((3,)))


def publish_body(dq_in, dk_in, dv_in, dq_out, dk_out, dv_out, sem):
    core = lax.rem(lax.axis_index("sp"), CORES)
    copies = [
        pltpu.make_async_copy(src.at[core], dst, sem.at[i])
        for i, (src, dst) in enumerate(((dq_in, dq_out), (dk_in, dk_out), (dv_in, dv_out)))
    ]
    for copy in copies:
        copy.start()
    for copy in copies:
        copy.wait()


def on_pairs(query_rows, key_rows, value_rows, out_grad, question_lengths):
    tokens = query_rows.shape[0]
    heads = KVH // CORES
    group = QH // KVH
    rows = tokens * CORES
    low, wide = jnp.bfloat16, jnp.float32
    vmem, sems = pltpu.VMEM, lambda *shape: pltpu.SemaphoreType.DMA(shape)
    anywhere = pl.BlockSpec(memory_space=pl.ANY)
    tiles = group * CORES // 2
    grads = pl.pallas_call(
        partial(pair_kernel, tokens, heads, group),
        out_shape=tuple(
            pltpu.VMEM((CORES,) + array.shape, low) for array in (query_rows, key_rows, value_rows)
        ),
        in_specs=[anywhere] * 5,
        out_specs=(pl.BlockSpec(memory_space=pltpu.VMEM),) * 3,
        scratch_shapes=[
            vmem((CORES,) + query_rows.shape, low),
            vmem((CORES,) + query_rows.shape, low),
            vmem((CORES,) + key_rows.shape, low),
            vmem((CORES,) + key_rows.shape, low),
            vmem((heads, rows, HD), low),
            vmem((heads, rows, HD), low),
            vmem((rows, rows), wide),
            vmem((tiles, 2 * rows, rows), wide),
            vmem((tiles, HD, rows), wide),
            vmem((2 * tiles, 2 * rows, HD), low),
            vmem((2 * tiles, 2 * rows, HD), low),
            vmem((2 * tiles, HD, HD), low),
            vmem((tiles, rows, HD), low),
            vmem((HD, 2 * rows), low),
            vmem((tiles, 8, rows), wide),
            vmem((tiles, 8, rows), wide),
            vmem((2, CORES, heads, tokens, HD), wide),
            vmem((2, heads, tokens, HD), wide),
            vmem((2, heads, rows, HD), low),
            vmem((2, CORES, heads, tokens, HD), low),
            pltpu.SMEM(question_lengths.shape, jnp.int32),
        ],
        compiler_params=pltpu.CompilerParams(
            collective_id=0, has_side_effects=True,
        ),
    )(question_lengths, query_rows, out_grad, key_rows, value_rows)
    return pl.pallas_call(
        publish_kernel,
        out_shape=tuple(
            jax.ShapeDtypeStruct(array.shape, low) for array in (query_rows, key_rows, value_rows)
        ),
        in_specs=[anywhere] * 3,
        out_specs=(anywhere,) * 3,
        compiler_params=pltpu.CompilerParams(has_side_effects=True, vmem_limit_bytes=1024 * 1024),
    )(*grads)


def solution(mesh):
    body = on_pairs if mesh.shape["sp"] == 2 * CORES else on_device
    return jax.shard_map(
        body,
        mesh=mesh,
        in_specs=(
            P(("grp", "sp"), None),
            P(("grp", "sp"), None),
            P(("grp", "sp"), None),
            P(("grp", "sp"), None),
            P("grp"),
        ),
        out_specs=(P(("grp", "sp"), None), P(("grp", "sp"), None), P(("grp", "sp"), None)),
        check_vma=False,
    )
```
